128 devices in a mesh: dp: 4 (over z_lo, core), ulysses: 4 (over y), expert: 8 (over x, z_hi).
Axes of the slice: x: 4, y: 4, z: 4 (z_hi: 2, z_lo: 2; z = z_hi * 2 + z_lo), core: 2. Of those that a mesh axis runs over, the one named last changes fastest.
Arguments:
- residual: bfloat16 [16384, 4096], P(('dp', 'ulysses', 'expert')), may hold values from -24 to 24
- norm_gain: float32 [4096], replicated, may hold values from 0.1 to 1.9
- grad_out: bfloat16 [16384, 4096], P(('dp', 'ulysses', 'expert')), may hold values from -24 to 24
- expert_ids: int32 [16384, 2], P(('dp', 'ulysses', 'expert')), may hold values from 0 to 7, all different within a row; in each aligned block of 128 rows (0 to 127, 128 to 255, ...) at most 48 rows name the same one
- route_weights: bfloat16 [16384, 2], P(('dp', 'ulysses', 'expert')), may hold values from 0.099609375 to 1
- weight_in: bfloat16 [8, 4096, 1536], P('expert'), may hold values from -0.09375 to 0.09375
- weight_down: bfloat16 [8, 768, 4096], P('expert'), may hold values from -0.21875 to 0.21875
Outputs:
- grad_residual: bfloat16 [16384, 4096], P(('dp', 'ulysses', 'expert'))
- route_grad: bfloat16 [16384, 2], P(('dp', 'ulysses', 'expert'))
- grad_in: float32 [8, 4096, 1536], P('expert', ('dp', 'ulysses'))
- grad_down: float32 [8, 4096, 768], P('expert', ('dp', 'ulysses'))
The draws below stay inside these ranges and needn't reach their ends.
Inputs may be any that keep to these rules, and one draw needn't show every extreme that they name: `expert_ids`: each row names 2 different experts. Among the rows of one device no expert is named more than 48 times, and in some devices' rows one expert is named exactly 48 times.
All inputs are finite; a program needn't handle non-finite values.
Results may differ from the reference program's by a relative error of at most 0.017.
Values may be sent and summed in bfloat16 or wider, within the bound.
No kernel may reach another device: no remote copies, remote signals or barrier semaphores. Data moves between devices by JAX's collectives and lax.ppermute only.
A program may use at most 192 MiB of HBM per device.

```python
import math
import jax
import jax.numpy as jnp
import numpy as np
from jax import lax

D = 4096
HID = 768
TOPK = 2
TOK_DEV = 128
EXPERTS = 8
TOKENS = 16384
CAP = 48
N_DP = 4
N_ULYSSES = 4
N_EXPERT = 8
DEVICES = 128


def raised(array, rng, source, target, shards_of, factor):
    def block_of(axis_at):
        return (jnp.arange(array.shape[axis_at]) // (array.shape[axis_at] // shards_of)).reshape((-1,) + (1,) * (array.ndim - 1 - axis_at))

    one_side = jax.random.permutation(rng, shards_of)[block_of(target)]
    far = (block_of(target) + shards_of // 2) % shards_of
    return jnp.where((block_of(source) == one_side) | (block_of(source) == far), factor * array, array)


def shard_levels(stream_key, extent, cuts, least, top_value):
    gain = 1.0
    for dim, parts in cuts:
        draws = jax.random.uniform(jax.random.fold_in(jax.random.fold_in(stream_key, 6), dim), (parts,), jnp.float32, least / len(cuts), top_value / len(cuts))
        gain = gain * jnp.repeat(jnp.exp(draws), extent[dim] // parts).reshape((-1,) + (1,) * (len(extent) - 1 - dim))
    return gain


def shared_out(stream_key, own, number, rows, count, top, limit, skew):
    ranking = jax.random.permutation(stream_key, count)
    crowded, ordinary = portions_of(count, rows * top, limit, skew, True), portions_of(count, rows * top, limit, skew, False)
    places = jnp.arange(count)

    def named(lengths, turn):
        used = int((lengths > 0).sum())
        fixed = max(1, used // 4)
        moved = fixed + (places - fixed + turn * (used - fixed)) % max(1, count - fixed)
        return jnp.zeros((count,), jnp.int32).at[ranking[jnp.where(places < fixed, places, moved)]].set(jnp.asarray(lengths, jnp.int32))

    lengths = jnp.where(number % 4 == 0, named(crowded, number // 4), named(ordinary, number - number // 4 - 1))
    mixed = jax.random.permutation(jax.random.fold_in(own, 3), count)
    source_of, receiver = mixed[0:count // 2 * 2:2], mixed[1:count // 2 * 2:2]
    room = jnp.minimum(lengths[source_of] - 1, limit - lengths[receiver]) // 2
    room = jnp.where((source_of == ranking[0]) | (receiver == ranking[0]) | (lengths[receiver] == 0), 0, jnp.maximum(room, 0))
    moved = jax.random.randint(jax.random.fold_in(own, 4), (count // 2,), 0, 1 << 20) % (room + 1)
    lengths = lengths.at[source_of].add(-moved).at[receiver].add(moved)
    labels = jnp.searchsorted(jnp.cumsum(lengths), jnp.arange(rows * top), side="right").astype(jnp.int32)
    listing = labels.reshape(top, rows).T
    listing = listing[jax.random.permutation(jax.random.fold_in(own, 1), rows)]
    turn = jax.random.randint(jax.random.fold_in(own, 2), (rows, 1), 0, top)
    return jnp.take_along_axis(listing, (jnp.arange(top)[None, :] + turn) % top, axis=1)


def portions_of(amount, total, most, skew, full):
    portions = [(1 << 20) // math.isqrt(standing ** skew) + 1 for standing in range(1, amount + 1)]
    largest = most if full else min(most, max(-(-total // amount), total * portions[0] // sum(portions)))
    least = 1 if total - largest >= amount - 1 else 0
    holding, rest = [largest] + [least] * (amount - 1), total - largest - least * (amount - 1)
    while rest > 0:
        candidates = [i for i in range(1, amount) if holding[i] < largest] or [i for i in range(1, amount) if holding[i] < most]
        pool, remaining = sum([portions[i] for i in candidates]), rest
        for i in candidates:
            more = min(most - holding[i], max(1, remaining * portions[i] // pool), rest)
            holding[i] = holding[i] + more
            rest = rest - more
    return np.array(holding)


def gaussian(stream_key, extent, spread, most, split=(), kind=jnp.bfloat16):
    entries = jax.random.normal(stream_key, extent, jnp.float32) * spread
    if len(split) > 0:
        entries = shard_levels(stream_key, extent, split, -0.22, 0.18) * entries
    return jnp.clip(entries, min=-most, max=most).astype(kind)


def heavy_noise(own_key, shape, width, limit, split, heavy, kind=jnp.bfloat16):
    array = width * jax.random.normal(own_key, shape, jnp.float32)
    if split:
        array = array * shard_levels(own_key, shape, split, -0.22, 0.18)
    return jnp.clip(raised(array, jax.random.fold_in(own_key, 3), *heavy), -limit, limit).astype(kind)


def setup_inputs(seed: int = 0) -> dict:
    seeds = jax.random.split(jax.random.key(seed), 8)
    residual = heavy_noise(seeds[0], (TOKENS, D), 1.0, 24.0, ((0, 128),), (0, 1, 128, 5.5))
    norm_gain = jnp.clip(1.0 + 0.18 * jax.random.normal(seeds[1], (D,), jnp.float32), 0.1, 1.9)
    grad_out = heavy_noise(seeds[2], (TOKENS, D), 1.0, 24.0, ((0, 128),), (0, 1, 128, 5.5))
    expert_ids_keys = jax.random.split(jax.random.fold_in(seeds[3], 1), TOKENS // TOK_DEV)
    expert_ids_turns = jax.random.permutation(jax.random.fold_in(seeds[3], 3), TOKENS // TOK_DEV)
    expert_ids = jax.vmap(lambda own, number: shared_out(jax.random.fold_in(seeds[3], 2), own, number, TOK_DEV, EXPERTS, TOPK, CAP, 2))(expert_ids_keys, expert_ids_turns).reshape((TOKENS, TOPK))
    route_weights = jnp.clip(0.099609375 + 0.9003906 * jax.random.uniform(seeds[4], (TOKENS, TOPK), jnp.float32) ** shard_levels(seeds[4], (TOKENS, TOPK), ((0, 128),), -0.2, 0.2), 0.099609375, 1.0).astype(jnp.bfloat16)
    weight_in = gaussian(seeds[5], (EXPERTS, D, 2 * HID), D ** -0.5, 0.09375, ((0, 8),))
    weight_down = gaussian(seeds[6], (EXPERTS, HID, D), HID ** -0.5, 0.21875, ((0, 8),))
    return dict(residual=residual, norm_gain=norm_gain, grad_out=grad_out, expert_ids=expert_ids, route_weights=route_weights, weight_in=weight_in, weight_down=weight_down)


eps = 1e-06

def slot_positions(expert_ids):
    flat_ids = expert_ids.reshape(DEVICES, TOK_DEV * TOPK).astype(jnp.int32)
    one_hot = (flat_ids[:, :, None] == jnp.arange(EXPERTS, dtype=jnp.int32)[None, None, :]).astype(jnp.int32)
    ranks = jnp.cumsum(one_hot, axis=1) - one_hot
    slots = lax.optimization_barrier(jnp.sum(ranks * one_hot, axis=2)).astype(jnp.int32)
    blocks = (jnp.arange(DEVICES, dtype=jnp.int32) % N_EXPERT)[:, None]
    return (flat_ids * (N_EXPERT * CAP) + blocks * CAP + slots).astype(jnp.int32)

def reference(residual, norm_gain, grad_out, expert_ids, route_weights, weight_in, weight_down):
    groups = N_DP * N_ULYSSES
    members = N_EXPERT * TOK_DEV
    slots_all = EXPERTS * N_EXPERT * CAP
    resid = residual.astype(jnp.float32)
    inv_rms = lax.rsqrt(lax.optimization_barrier(jnp.mean(resid * resid, axis=-1, keepdims=True)) + eps)
    unit_rows = resid * inv_rms
    normed = (unit_rows * norm_gain).astype(jnp.bfloat16)
    positions = slot_positions(expert_ids).reshape(groups, members * TOPK)
    token_local = (jnp.arange(members * TOPK, dtype=jnp.int32) // TOPK).astype(jnp.int32)
    weights_grouped = route_weights.reshape(groups, members * TOPK)
    normed_grouped = normed.reshape(groups, members, D)
    grad_grouped = grad_out.reshape(groups, members, D)
    win = weight_in.astype(jnp.float32)
    wdown = weight_down.astype(jnp.float32)

    def group_step(carry, inputs):
        acc_in, acc_down = carry
        where, weights, normed_rows, grad_rows = inputs
        source = jnp.full((slots_all,), members, jnp.int32).at[where].set(token_local)
        slot_weight = jnp.zeros((slots_all,), jnp.bfloat16).at[where].set(weights)
        padded_normed = jnp.concatenate([normed_rows, jnp.zeros((1, D), jnp.bfloat16)], 0)
        padded_grad = jnp.concatenate([grad_rows, jnp.zeros((1, D), jnp.bfloat16)], 0)
        sent_normed = padded_normed[source].reshape(EXPERTS, N_EXPERT * CAP, D).astype(jnp.float32)
        sent_grad = padded_grad[source].reshape(EXPERTS, N_EXPERT * CAP, D).astype(jnp.float32)
        slot_col = slot_weight.reshape(EXPERTS, N_EXPERT * CAP, 1).astype(jnp.float32)
        proj = jnp.einsum('erd,edh->erh', sent_normed, win)
        gate_proj = proj[..., :HID]
        up_proj = proj[..., HID:]
        sigmoid_gate = jax.nn.sigmoid(gate_proj)
        silu_gate = gate_proj * sigmoid_gate
        hidden = lax.optimization_barrier((silu_gate * up_proj).astype(jnp.bfloat16)).astype(jnp.float32)
        back_proj = jnp.einsum('erd,ehd->erh', sent_grad, wdown)
        slot_grad = lax.optimization_barrier(jnp.sum(back_proj * hidden, axis=-1)).astype(jnp.bfloat16)
        grad_hidden = slot_col * back_proj
        d_gate = grad_hidden * up_proj * sigmoid_gate * (1.0 + gate_proj * (1.0 - sigmoid_gate))
        d_up = grad_hidden * silu_gate
        d_proj = lax.optimization_barrier(jnp.concatenate([d_gate, d_up], -1).astype(jnp.bfloat16)).astype(jnp.float32)
        slot_normed = jnp.einsum('erh,edh->erd', d_proj, win).astype(jnp.bfloat16)
        scaled = lax.optimization_barrier((slot_col * sent_grad).astype(jnp.bfloat16)).astype(jnp.float32)
        part_in = lax.optimization_barrier(jnp.einsum('erd,erh->edh', sent_normed, d_proj).astype(jnp.bfloat16)).astype(jnp.float32)
        part_down = lax.optimization_barrier(jnp.einsum('erd,erh->edh', scaled, hidden).astype(jnp.bfloat16)).astype(jnp.float32)
        flat_normed = slot_normed.reshape(slots_all, D).astype(jnp.float32)
        token_normed = lax.optimization_barrier(jnp.sum(flat_normed[where].reshape(members, TOPK, D), axis=1))
        token_route = slot_grad.reshape(slots_all)[where].reshape(members, TOPK)
        return ((acc_in + part_in, acc_down + part_down), (token_normed, token_route))
    init = (jnp.zeros((EXPERTS, D, 2 * HID), jnp.float32), jnp.zeros((EXPERTS, D, HID), jnp.float32))
    (grad_in, grad_down), (grad_normed, route_grad) = lax.scan(group_step, init, (positions, weights_grouped, normed_grouped, grad_grouped))
    grad_normed = grad_normed.reshape(TOKENS, D)
    scaled_normed = grad_normed * norm_gain
    branch = inv_rms * (scaled_normed - unit_rows * lax.optimization_barrier(jnp.mean(scaled_normed * unit_rows, axis=-1, keepdims=True)))
    grad_residual = (grad_out.astype(jnp.float32) + branch).astype(jnp.bfloat16)
    return (grad_residual, route_grad.reshape(TOKENS, TOPK), grad_in, grad_down)
```

```python
import jax
import jax.numpy as jnp
from jax import lax
from jax.sharding import Mesh
from jax.sharding import PartitionSpec as P

DP_ULYSSES = ("dp_0", "dp_1", "ulysses")
DP_ULYSSES_EXPERT = ("dp_0", "dp_1", "ulysses", "expert")

SWAP = [(0, 1), (1, 0)]

eps = 1e-06


def contract_rows(left, right):
    return lax.dot_general(
        left, right, (((0,), (0,)), ((), ())), preferred_element_type=jnp.float32
    )


def contract_cols(left, right):
    return lax.dot_general(
        left, right, (((1,), (1,)), ((), ())), preferred_element_type=jnp.float32
    )


def slot_tables(ids_t, weights_t, experts, capacity):
    tok_rows = ids_t.shape[1]
    lanes = (experts, tok_rows)
    chosen = ids_t[:, None, :] == lax.broadcasted_iota(jnp.int32, (1, experts, tok_rows), 1)
    hit = jnp.any(chosen, axis=0)
    weight = jnp.sum(jnp.where(chosen, weights_t[:, None, :].astype(jnp.float32), 0.0), axis=0)
    square = (tok_rows, tok_rows)
    before = lax.broadcasted_iota(jnp.int32, square, 0) < lax.broadcasted_iota(jnp.int32, square, 1)
    rank = jnp.dot(
        hit.astype(jnp.bfloat16), before.astype(jnp.bfloat16), preferred_element_type=jnp.float32
    )
    rank = jnp.where(hit, rank.astype(jnp.int32), capacity)
    slot = lax.broadcasted_iota(jnp.int32, (1, capacity, 1), 1)
    held = rank[:, None, :] == slot
    select = jnp.where(held, 1.0, 0.0).astype(jnp.bfloat16).reshape(-1, tok_rows)
    scale = jnp.where(held, weight[:, None, :], 0.0).astype(jnp.bfloat16).reshape(-1, tok_rows)
    return chosen, select, scale


def per_device(residual, norm_gain, grad_out, expert_ids, route_weights, weight_in, weight_down):
    tok_rows, width = residual.shape
    topk = expert_ids.shape[1]
    hidden_width = weight_down.shape[1]
    experts = lax.axis_size("expert")
    capacity = min(tok_rows, 3 * tok_rows * topk // (2 * experts))
    slot_total = experts * capacity
    rings = lax.axis_size("ulysses")
    stretch = width // (lax.axis_size("dp_0") * lax.axis_size("dp_1"))
    resid = residual.astype(jnp.float32)
    inv_rms = lax.rsqrt(jnp.mean(resid * resid, axis=-1, keepdims=True) + eps)
    unit_rows = resid * inv_rms
    normed = (unit_rows * norm_gain).astype(jnp.bfloat16)
    weights_t = route_weights.T
    chosen, select, scale = slot_tables(expert_ids.T, weights_t, experts, capacity)
    send_normed = jnp.dot(select, normed, preferred_element_type=jnp.float32).astype(jnp.bfloat16)
    send_scaled = jnp.dot(scale, grad_out, preferred_element_type=jnp.float32).astype(jnp.bfloat16)
    send = jnp.concatenate([send_normed, send_scaled], axis=1)
    got = lax.all_to_all(
        send.reshape(experts, capacity, 2 * width), "expert", split_axis=0, concat_axis=0, tiled=True
    ).reshape(slot_total, 2 * width)
    rows_normed = got[:, :width]
    rows_scaled = got[:, width:]
    w_in = weight_in[0]
    w_down = weight_down[0]
    proj = jnp.dot(rows_normed, w_in, preferred_element_type=jnp.float32)
    gate_proj = proj[:, :hidden_width]
    up_proj = proj[:, hidden_width:]
    sigmoid_gate = jax.nn.sigmoid(gate_proj)
    silu_gate = gate_proj * sigmoid_gate
    hidden = (silu_gate * up_proj).astype(jnp.bfloat16)
    grad_hidden = contract_cols(rows_scaled, w_down)
    slot_grad = jnp.sum(grad_hidden * hidden.astype(jnp.float32), axis=1).astype(jnp.bfloat16)
    d_gate = grad_hidden * up_proj * sigmoid_gate * (1.0 + gate_proj * (1.0 - sigmoid_gate))
    d_up = grad_hidden * silu_gate
    d_proj = jnp.concatenate([d_gate, d_up], axis=1).astype(jnp.bfloat16)

    side = lax.axis_index("dp_0")
    core = lax.axis_index("dp_1")

    def columns(rows, half, quarter):
        return lax.dynamic_slice_in_dim(rows, (half * 2 + quarter) * stretch, stretch, axis=1)

    def core_sum(rows, right, half):
        give = contract_rows(columns(rows, half, 1 - core), right).astype(jnp.bfloat16)
        came = lax.ppermute(give, "dp_1", SWAP)
        keep = contract_rows(columns(rows, half, core), right)
        return (keep + came.astype(jnp.float32)).astype(jnp.bfloat16)

    def ring_sum(rows, right, half):
        part = core_sum(rows, right, half)
        return lax.psum_scatter(part, "ulysses", scatter_dimension=0, tiled=True)

    far_down = ring_sum(rows_scaled, hidden, 1 - side)
    far_in = ring_sum(rows_normed, d_proj, 1 - side)
    near_down = ring_sum(rows_scaled, hidden, side)
    near_in = ring_sum(rows_normed, d_proj, side)
    came_down = lax.ppermute(far_down, "dp_0", SWAP)
    came_in = lax.ppermute(far_in, "dp_0", SWAP)
    grad_down = (near_down.astype(jnp.float32) + came_down.astype(jnp.float32))[None]
    grad_in = (near_in.astype(jnp.float32) + came_in.astype(jnp.float32))[None]

    slot_normed = contract_cols(d_proj, w_in).astype(jnp.bfloat16)
    back_normed = lax.all_to_all(
        slot_normed.reshape(experts, capacity, width),
        "expert",
        split_axis=0,
        concat_axis=0,
        tiled=True,
    )
    back_route = lax.all_to_all(
        slot_grad.reshape(experts, capacity), "expert", split_axis=0, concat_axis=0, tiled=True
    )
    grad_normed = contract_rows(select, back_normed.reshape(slot_total, width))
    token_route = jnp.sum(
        select.reshape(experts, capacity, tok_rows).astype(jnp.float32)
        * back_route.astype(jnp.float32)[:, :, None],
        axis=1,
    )
    route_t = jnp.sum(jnp.where(chosen, token_route[None], 0.0), axis=1)
    route_grad = (route_t / weights_t.astype(jnp.float32)).astype(jnp.bfloat16).T
    scaled_normed = grad_normed * norm_gain
    branch = inv_rms * (
        scaled_normed - unit_rows * jnp.mean(scaled_normed * unit_rows, axis=-1, keepdims=True)
    )
    grad_residual = (grad_out.astype(jnp.float32) + branch).astype(jnp.bfloat16)
    return (grad_residual, route_grad, grad_in, grad_down)


def solution(mesh):
    finer = Mesh(
        mesh.devices.reshape(2, 2, mesh.shape["ulysses"], mesh.shape["expert"]),
        ("dp_0", "dp_1", "ulysses", "expert"),
    )
    return jax.shard_map(
        per_device,
        mesh=finer,
        in_specs=(
            P(DP_ULYSSES_EXPERT, None),
            P(),
            P(DP_ULYSSES_EXPERT, None),
            P(DP_ULYSSES_EXPERT, None),
            P(DP_ULYSSES_EXPERT, None),
            P("expert", None, None),
            P("expert", None, None),
        ),
        out_specs=(
            P(DP_ULYSSES_EXPERT, None),
            P(DP_ULYSSES_EXPERT, None),
            P("expert", DP_ULYSSES, None),
            P("expert", DP_ULYSSES, None),
        ),
        check_vma=False,
    )
```

```python
import jax
import jax.numpy as jnp
from jax import lax
from jax.experimental import pallas as pl
from jax.experimental.pallas import tpu as pltpu
from jax.sharding import Mesh
from jax.sharding import PartitionSpec as P

DP_ULYSSES = ("dp_0", "dp_1", "ulysses")
DP_ULYSSES_EXPERT = ("dp_0", "dp_1", "ulysses", "expert")

SWAP = [(0, 1), (1, 0)]

eps = 1e-06


def contract(left, right, over_left, over_right):
    return lax.dot_general(
        left, right, (((over_left,), (over_right,)), ((), ())), preferred_element_type=jnp.float32
    )


def slot_matrices(ids, weights, experts, capacity):
    tok_rows = ids.shape[1]
    expert = lax.broadcasted_iota(jnp.int32, (experts, tok_rows), 0)
    first, second = ids[0:1] == expert, ids[1:2] == expert
    hit = first | second
    weight = jnp.where(first, weights[0:1], jnp.where(second, weights[1:2], 0.0))
    square = (tok_rows, tok_rows)
    before = lax.broadcasted_iota(jnp.int32, square, 0) < lax.broadcasted_iota(jnp.int32, square, 1)
    rank = contract(
        jnp.where(hit, 1.0, 0.0).astype(jnp.bfloat16),
        jnp.where(before, 1.0, 0.0).astype(jnp.bfloat16),
        1,
        0,
    ).astype(jnp.int32)
    rank = jnp.where(hit, rank, capacity)
    slot = lax.broadcasted_iota(jnp.int32, (capacity, tok_rows), 0)
    select, scale = [], []
    for e in range(experts):
        held = rank[e : e + 1] == slot
        select.append(jnp.where(held, 1.0, 0.0))
        scale.append(jnp.where(held, weight[e : e + 1], 0.0))
    return (
        jnp.concatenate(select, axis=0).astype(jnp.bfloat16),
        jnp.concatenate(scale, axis=0).astype(jnp.bfloat16),
    )


def pack_kernel(ids_ref, w_ref, gain_ref, resid_ref, grad_ref, out_ref, sel_ref, inv_ref, scale_ref):
    experts, _, capacity, block = out_ref.shape

    @pl.when(pl.program_id(0) == 0)
    def _():
        full = resid_ref[...].astype(jnp.float32)
        mean = jnp.mean(full * full, axis=-1, keepdims=True)
        inv_ref[...] = lax.rsqrt(mean + eps)
        select, scale = slot_matrices(ids_ref[...], w_ref[...].astype(jnp.float32), experts, capacity)
        sel_ref[...] = select
        scale_ref[...] = scale

    at = pl.ds(pl.multiple_of(pl.program_id(0) * block, block), block)
    unit = resid_ref[:, at].astype(jnp.float32) * inv_ref[...]
    normed = (unit * gain_ref[:, at]).astype(jnp.bfloat16)
    sent = contract(sel_ref[...], normed, 1, 0).astype(jnp.bfloat16)
    out_ref[:, 0] = sent.reshape(experts, capacity, block)
    sent = contract(scale_ref[...], grad_ref[:, at], 1, 0).astype(jnp.bfloat16)
    out_ref[:, 1] = sent.reshape(experts, capacity, block)


def pack(ids_t, w_t, gain, resid, grad, experts, capacity, block=512):
    rows, width = resid.shape
    whole = lambda a: pl.BlockSpec(a.shape, lambda j: (0,) * a.ndim)
    args = (ids_t, w_t, gain, resid, grad)
    slots = experts * capacity
    return pl.pallas_call(
        pack_kernel,
        grid=(width // block,),
        in_specs=[whole(a) for a in args],
        out_specs=[
            pl.BlockSpec((experts, 2, capacity, block), lambda j: (0, 0, 0, j)),
            pl.BlockSpec((slots, rows), lambda j: (0, 0)),
        ],
        out_shape=[
            jax.ShapeDtypeStruct((experts, 2, capacity, width), jnp.bfloat16),
            jax.ShapeDtypeStruct((slots, rows), jnp.bfloat16),
        ],
        scratch_shapes=[
            pltpu.VMEM((rows, 1), jnp.float32),
            pltpu.VMEM((slots, rows), jnp.bfloat16),
        ],
        compiler_params=pltpu.CompilerParams(vmem_limit_bytes=40 * 2**20),
        cost_estimate=pl.CostEstimate(
            flops=4 * slots * rows * width, bytes_accessed=4 * slots * width, transcendentals=0
        ),
        name="pack",
    )(*args)


def expert_kernel(got_ref, gate_w_ref, up_w_ref, down_w_ref, out_ref, route_ref, acc_ref):
    parts, _, capacity, width = got_ref.shape
    slots = parts * capacity
    normed = got_ref[:, 0].reshape(slots, width)
    gate = contract(normed, gate_w_ref[...], 1, 0)
    up = contract(normed, up_w_ref[...], 1, 0)
    grad_hidden = contract(got_ref[:, 1].reshape(slots, width), down_w_ref[...], 1, 1)
    sigmoid = jax.nn.sigmoid(gate)
    silu = gate * sigmoid
    hidden = (silu * up).astype(jnp.bfloat16)
    out_ref[0] = hidden
    out_ref[1] = (grad_hidden * up * sigmoid * (1.0 + gate * (1.0 - sigmoid))).astype(jnp.bfloat16)
    out_ref[2] = (grad_hidden * silu).astype(jnp.bfloat16)
    part = jnp.sum(grad_hidden * hidden.astype(jnp.float32), axis=1, keepdims=True)

    @pl.when(pl.program_id(0) == 0)
    def _():
        acc_ref[...] = part

    @pl.when(pl.program_id(0) > 0)
    def _():
        acc_ref[...] += part

    @pl.when(pl.program_id(0) == pl.num_programs(0) - 1)
    def _():
        route_ref[...] = jnp.broadcast_to(acc_ref[...], route_ref.shape).astype(jnp.bfloat16)


def expert(got, w_in, w_down, block=256):
    parts, _, capacity, width = got.shape
    slots = parts * capacity
    hidden_width = w_down.shape[0]
    steps = hidden_width // block
    return pl.pallas_call(
        expert_kernel,
        grid=(steps,),
        in_specs=[
            pl.BlockSpec(got.shape, lambda j: (0, 0, 0, 0)),
            pl.BlockSpec((width, block), lambda j: (0, j)),
            pl.BlockSpec((width, block), lambda j: (0, steps + j)),
            pl.BlockSpec((block, width), lambda j: (j, 0)),
        ],
        out_specs=[
            pl.BlockSpec((3, slots, block), lambda j: (0, 0, j)),
            pl.BlockSpec((slots, 128), lambda j: (0, 0)),
        ],
        out_shape=[
            jax.ShapeDtypeStruct((3, slots, hidden_width), jnp.bfloat16),
            jax.ShapeDtypeStruct((slots, 128), jnp.bfloat16),
        ],
        scratch_shapes=[pltpu.VMEM((slots, 1), jnp.float32)],
        compiler_params=pltpu.CompilerParams(vmem_limit_bytes=58 * 2**20),
        cost_estimate=pl.CostEstimate(
            flops=6 * slots * hidden_width * width,
            bytes_accessed=6 * hidden_width * width + 4 * slots * width,
            transcendentals=slots * hidden_width,
        ),
        name="expert",
    )(got, w_in, w_in, w_down)


def weight_block(own_ref, far_ref, near_ref, mine_ref, theirs_ref, units):
    slots = mine_ref.shape[1]
    own = own_ref[:, 0].reshape(slots, -1)
    came = jnp.where(pl.program_id(0) == 0, far_ref[:, 0], near_ref[:, 0]).reshape(slots, -1)
    return [
        contract(own, mine_ref[u], 0, 0) + contract(came, theirs_ref[u], 0, 0) for u in units
    ]


def grad_in_kernel(_, own_ref, far_ref, near_ref, mine_ref, theirs_ref, out_ref):
    gate, up = weight_block(own_ref, far_ref, near_ref, mine_ref, theirs_ref, (1, 2))
    width = gate.shape[1]
    out_ref[0, 0, :, :width] = gate.astype(jnp.bfloat16)
    out_ref[0, 0, :, width:] = up.astype(jnp.bfloat16)


def grad_down_kernel(_, own_ref, far_ref, near_ref, mine_ref, theirs_ref, far_out, near_out):
    (down,) = weight_block(own_ref, far_ref, near_ref, mine_ref, theirs_ref, (0,))
    down = down.astype(jnp.bfloat16)

    @pl.when(pl.program_id(0) == 0)
    def _():
        far_out[0] = down

    @pl.when(pl.program_id(0) == 1)
    def _():
        near_out[0] = down


def weight_grads(kernel, kind, units, place, got, far, near, mine, theirs, rings, out_specs, out_shape):
    parts, _, capacity, width = got.shape
    block = width // (4 * rings)
    slots, hidden_width = mine.shape[1:]
    stretch = (parts, 1, capacity, block)

    def own_at(half, ring, place_ref):
        side = jnp.where(half == 0, 1 - place_ref[0], place_ref[0])
        return (0, kind, 0, (side * 2 + place_ref[1]) * rings + ring)

    def far_at(half, ring, place_ref):
        return (0, kind, 0, jnp.where(half == 0, ring, rings - 1))

    def near_at(half, ring, place_ref):
        return (0, kind, 0, jnp.where(half == 0, 0, ring))

    whole = pl.BlockSpec(mine.shape, lambda half, ring, place_ref: (0, 0, 0))
    return pl.pallas_call(
        kernel,
        grid_spec=pltpu.PrefetchScalarGridSpec(
            num_scalar_prefetch=1,
            grid=(2, rings),
            in_specs=[
                pl.BlockSpec(stretch, own_at),
                pl.BlockSpec(stretch, far_at),
                pl.BlockSpec(stretch, near_at),
                whole,
                whole,
            ],
            out_specs=out_specs,
        ),
        out_shape=out_shape,
        compiler_params=pltpu.CompilerParams(vmem_limit_bytes=58 * 2**20),
        cost_estimate=pl.CostEstimate(
            flops=2 * slots * width * hidden_width * units,
            bytes_accessed=width * hidden_width * units + 2 * slots * width,
            transcendentals=0,
        ),
    )(place, got, far, near, mine, theirs)


def slot_kernel(grads_ref, w_ref, out_ref):
    width = grads_ref.shape[2]
    rows = contract(grads_ref[1], w_ref[:, :width], 1, 1) + contract(
        grads_ref[2], w_ref[:, width:], 1, 1
    )
    out_ref[...] = rows.astype(jnp.bfloat16).reshape(out_ref.shape)


def slot_rows(grads, w_in, parts, block=512):
    _, slots, hidden_width = grads.shape
    width = w_in.shape[0]
    return pl.pallas_call(
        slot_kernel,
        grid=(width // block,),
        in_specs=[
            pl.BlockSpec(grads.shape, lambda j: (0, 0, 0)),
            pl.BlockSpec((block, 2 * hidden_width), lambda j: (j, 0)),
        ],
        out_specs=pl.BlockSpec((parts, slots // parts, block), lambda j: (0, 0, j)),
        out_shape=jax.ShapeDtypeStruct((parts, slots // parts, width), jnp.bfloat16),
        compiler_params=pltpu.CompilerParams(vmem_limit_bytes=60 * 2**20),
        cost_estimate=pl.CostEstimate(
            flops=4 * slots * hidden_width * width,
            bytes_accessed=4 * hidden_width * width + 2 * slots * width,
            transcendentals=0,
        ),
        name="slot_rows",
    )(grads, w_in)


def per_device(residual, norm_gain, grad_out, expert_ids, route_weights, weight_in, weight_down):
    tok_rows, width = residual.shape
    topk = expert_ids.shape[1]
    hidden_width = weight_down.shape[1]
    experts = lax.axis_size("expert")
    capacity = min(tok_rows, 3 * tok_rows * topk // (2 * experts))
    slot_total = experts * capacity
    rings = lax.axis_size("ulysses")
    quarter = width // 4
    block = quarter // rings
    side = lax.axis_index("dp_0")
    core = lax.axis_index("dp_1")
    ids_t = expert_ids.T
    weights_t = route_weights.T
    place, residual = lax.optimization_barrier(
        (jnp.stack([side, core]).astype(jnp.int32), residual)
    )
    side, core = place[0], place[1]

    send, select = pack(ids_t, weights_t, norm_gain[None], residual, grad_out, experts, capacity)
    got = lax.all_to_all(
        send.reshape(experts, 2 * capacity, width),
        "expert",
        split_axis=0,
        concat_axis=0,
        tiled=True,
    )
    (got, place, ids_t, weights_t, residual, grad_out, norm_gain, weight_in, weight_down, select) = (
        lax.optimization_barrier(
            (got, place, ids_t, weights_t, residual, grad_out, norm_gain, weight_in, weight_down, select)
        )
    )
    side, core = place[0], place[1]
    got = got.reshape(experts, 2, capacity, width)
    w_in = weight_in[0]
    w_down = weight_down[0]

    def swap_cores(half):
        start = (half * 2 + 1 - core) * quarter
        return lax.ppermute(lax.dynamic_slice_in_dim(got, start, quarter, axis=3), "dp_1", SWAP)

    far = swap_cores(1 - side)
    near = swap_cores(side)
    mine, route = expert(got, w_in, w_down)
    theirs = lax.ppermute(mine, "dp_1", SWAP)
    shared = (place, got, far, near, mine, theirs, rings)
    part_in = weight_grads(
        grad_in_kernel,
        0,
        2,
        *shared,
        pl.BlockSpec((1, 1, block, 2 * hidden_width), lambda half, ring, _: (ring, half, 0, 0)),
        jax.ShapeDtypeStruct((rings, 2, block, 2 * hidden_width), jnp.bfloat16),
    )
    far_down, near_down = weight_grads(
        grad_down_kernel,
        1,
        1,
        *shared,
        [
            pl.BlockSpec(
                (1, block, hidden_width),
                lambda half, ring, _: (jnp.where(half == 0, ring, rings - 1), 0, 0),
            ),
            pl.BlockSpec(
                (1, block, hidden_width), lambda half, ring, _: (jnp.where(half == 0, 0, ring), 0, 0)
            ),
        ],
        [jax.ShapeDtypeStruct((rings, block, hidden_width), jnp.bfloat16)] * 2,
    )
    came_down = lax.ppermute(far_down, "dp_0", SWAP)
    summed_in = lax.psum_scatter(
        part_in.reshape(rings, 2 * block, 2 * hidden_width),
        "ulysses",
        scatter_dimension=0,
        tiled=True,
    )[0]
    came_in = lax.ppermute(summed_in[:block], "dp_0", SWAP)
    grad_in = (summed_in[block:].astype(jnp.float32) + came_in.astype(jnp.float32))[None]
    part_down = (near_down.astype(jnp.float32) + came_down.astype(jnp.float32)).astype(jnp.bfloat16)
    summed_down = lax.psum_scatter(part_down, "ulysses", scatter_dimension=0, tiled=True)
    grad_down = summed_down.astype(jnp.float32)

    back_normed = lax.all_to_all(
        slot_rows(mine, w_in, experts), "expert", split_axis=0, concat_axis=0, tiled=True
    )
    back_route = lax.all_to_all(
        route[:, 0].reshape(experts, capacity), "expert", split_axis=0, concat_axis=0, tiled=True
    )
    resid = residual.astype(jnp.float32)
    inv_rms = lax.rsqrt(jnp.mean(resid * resid, axis=-1, keepdims=True) + eps)
    unit_rows = resid * inv_rms
    grad_normed = contract(select, back_normed.reshape(slot_total, width), 0, 0)
    token_route = jnp.sum(
        select.reshape(experts, capacity, tok_rows).astype(jnp.float32)
        * back_route.astype(jnp.float32)[:, :, None],
        axis=1,
    )
    chosen = ids_t[:, None, :] == lax.broadcasted_iota(jnp.int32, (1, experts, tok_rows), 1)
    route_t = jnp.sum(jnp.where(chosen, token_route[None], 0.0), axis=1)
    route_grad = (route_t / weights_t.astype(jnp.float32)).astype(jnp.bfloat16).T
    scaled_normed = grad_normed * norm_gain
    branch = inv_rms * (
        scaled_normed - unit_rows * jnp.mean(scaled_normed * unit_rows, axis=-1, keepdims=True)
    )
    grad_residual = (grad_out.astype(jnp.float32) + branch).astype(jnp.bfloat16)
    return (grad_residual, route_grad, grad_in, grad_down)


def solution(mesh):
    finer = Mesh(
        mesh.devices.reshape(2, 2, mesh.shape["ulysses"], mesh.shape["expert"]),
        ("dp_0", "dp_1", "ulysses", "expert"),
    )
    return jax.shard_map(
        per_device,
        mesh=finer,
        in_specs=(
            P(DP_ULYSSES_EXPERT, None),
            P(),
            P(DP_ULYSSES_EXPERT, None),
            P(DP_ULYSSES_EXPERT, None),
            P(DP_ULYSSES_EXPERT, None),
            P("expert", None, None),
            P("expert", None, None),
        ),
        out_specs=(
            P(DP_ULYSSES_EXPERT, None),
            P(DP_ULYSSES_EXPERT, None),
            P("expert", DP_ULYSSES, None),
            P("expert", DP_ULYSSES, None),
        ),
        check_vma=False,
    )
```

```python
import jax
import jax.numpy as jnp
from jax import lax
from jax.experimental import pallas as pl
from jax.experimental.pallas import tpu as pltpu
from jax.sharding import Mesh
from jax.sharding import PartitionSpec as P

DP_ULYSSES = ("dp_0", "dp_1", "ulysses")
DP_ULYSSES_EXPERT = ("dp_0", "dp_1", "ulysses", "expert")

SWAP = [(0, 1), (1, 0)]

eps = 1e-06

VMEM = 62 * 2**20


def contract(left, right, over_left, over_right):
    return lax.dot_general(
        left, right, (((over_left,), (over_right,)), ((), ())), preferred_element_type=jnp.float32
    )


def slot_matrices(ids, weights, experts, capacity):
    tok_rows = ids.shape[1]
    expert = lax.broadcasted_iota(jnp.int32, (experts, tok_rows), 0)
    first, second = ids[0:1] == expert, ids[1:2] == expert
    hit = first | second
    weight = jnp.where(first, weights[0:1], jnp.where(second, weights[1:2], 0.0))
    square = (tok_rows, tok_rows)
    before = lax.broadcasted_iota(jnp.int32, square, 0) < lax.broadcasted_iota(jnp.int32, square, 1)
    rank = contract(
        jnp.where(hit, 1.0, 0.0).astype(jnp.bfloat16),
        jnp.where(before, 1.0, 0.0).astype(jnp.bfloat16),
        1,
        0,
    ).astype(jnp.int32)
    rank = jnp.where(hit, rank, capacity)
    slot = lax.broadcasted_iota(jnp.int32, (capacity, tok_rows), 0)
    select, scale = [], []
    for e in range(experts):
        held = rank[e : e + 1] == slot
        select.append(jnp.where(held, 1.0, 0.0))
        scale.append(jnp.where(held, weight[e : e + 1], 0.0))
    return (
        jnp.concatenate(select, axis=0).astype(jnp.bfloat16),
        jnp.concatenate(scale, axis=0).astype(jnp.bfloat16),
    )


def pack_kernel(
    ids_ref, w_ref, gain_ref, resid_ref, grad_ref, normed_ref, scaled_ref, sel_ref, inv_ref, scale_ref
):
    experts, capacity, block = normed_ref.shape

    @pl.when(pl.program_id(0) == 0)
    def _():
        full = resid_ref[...].astype(jnp.float32)
        mean = jnp.mean(full * full, axis=-1, keepdims=True)
        inv_ref[...] = lax.rsqrt(mean + eps)
        select, scale = slot_matrices(ids_ref[...], w_ref[...].astype(jnp.float32), experts, capacity)
        sel_ref[...] = select
        scale_ref[...] = scale

    at = pl.ds(pl.multiple_of(pl.program_id(0) * block, block), block)
    unit = resid_ref[:, at].astype(jnp.float32) * inv_ref[...]
    normed = (unit * gain_ref[:, at]).astype(jnp.bfloat16)
    sent = contract(sel_ref[...], normed, 1, 0).astype(jnp.bfloat16)
    normed_ref[...] = sent.reshape(experts, capacity, block)
    sent = contract(scale_ref[...], grad_ref[:, at], 1, 0).astype(jnp.bfloat16)
    scaled_ref[...] = sent.reshape(experts, capacity, block)


def pack(ids_t, w_t, gain, resid, grad, experts, capacity, block=512):
    rows, width = resid.shape
    whole = lambda a: pl.BlockSpec(a.shape, lambda j: (0,) * a.ndim)
    args = (ids_t, w_t, gain, resid, grad)
    slots = experts * capacity
    return pl.pallas_call(
        pack_kernel,
        grid=(width // block,),
        in_specs=[whole(a) for a in args],
        out_specs=[
            pl.BlockSpec((experts, capacity, block), lambda j: (0, 0, j)),
            pl.BlockSpec((experts, capacity, block), lambda j: (0, 0, j)),
            pl.BlockSpec((slots, rows), lambda j: (0, 0)),
        ],
        out_shape=[
            jax.ShapeDtypeStruct((experts, capacity, width), jnp.bfloat16),
            jax.ShapeDtypeStruct((experts, capacity, width), jnp.bfloat16),
            jax.ShapeDtypeStruct((slots, rows), jnp.bfloat16),
        ],
        scratch_shapes=[
            pltpu.VMEM((rows, 1), jnp.float32),
            pltpu.VMEM((slots, rows), jnp.bfloat16),
        ],
        compiler_params=pltpu.CompilerParams(vmem_limit_bytes=VMEM),
        cost_estimate=pl.CostEstimate(
            flops=4 * slots * rows * width, bytes_accessed=4 * slots * width, transcendentals=0
        ),
        name="pack",
    )(*args)


def forward_kernel(got_ref, gate_w_ref, up_w_ref, hidden_ref, gate_ref, up_ref):
    parts, capacity, width = got_ref.shape
    normed = got_ref[...].reshape(parts * capacity, width)
    gate = contract(normed, gate_w_ref[...], 1, 0)
    up = contract(normed, up_w_ref[...], 1, 0)
    sigmoid = jax.nn.sigmoid(gate)
    silu = gate * sigmoid
    hidden_ref[...] = (silu * up).astype(jnp.bfloat16)
    gate_ref[...] = up * sigmoid * (1.0 + gate * (1.0 - sigmoid))
    up_ref[...] = silu


def forward(got, w_in, block=256):
    parts, capacity, width = got.shape
    slots = parts * capacity
    hidden_width = w_in.shape[1] // 2
    steps = hidden_width // block
    out = pl.BlockSpec((slots, block), lambda j: (0, j))
    return pl.pallas_call(
        forward_kernel,
        grid=(steps,),
        in_specs=[
            pl.BlockSpec(got.shape, lambda j: (0, 0, 0)),
            pl.BlockSpec((width, block), lambda j: (0, j)),
            pl.BlockSpec((width, block), lambda j: (0, steps + j)),
        ],
        out_specs=[out] * 3,
        out_shape=[
            jax.ShapeDtypeStruct((slots, hidden_width), t)
            for t in (jnp.bfloat16, jnp.float32, jnp.float32)
        ],
        compiler_params=pltpu.CompilerParams(vmem_limit_bytes=VMEM),
        cost_estimate=pl.CostEstimate(
            flops=4 * slots * hidden_width * width,
            bytes_accessed=4 * hidden_width * width + 2 * slots * width,
            transcendentals=slots * hidden_width,
        ),
        name="forward",
    )(got, w_in, w_in)


def back_kernel(got_ref, w_ref, hidden_ref, gate_ref, up_ref, out_ref, route_ref, acc_ref):
    parts, capacity, width = got_ref.shape
    grad_hidden = contract(got_ref[...].reshape(parts * capacity, width), w_ref[...], 1, 1)
    out_ref[0] = (grad_hidden * gate_ref[...]).astype(jnp.bfloat16)
    out_ref[1] = (grad_hidden * up_ref[...]).astype(jnp.bfloat16)
    part = jnp.sum(grad_hidden * hidden_ref[...].astype(jnp.float32), axis=1, keepdims=True)

    @pl.when(pl.program_id(0) == 0)
    def _():
        acc_ref[...] = part

    @pl.when(pl.program_id(0) > 0)
    def _():
        acc_ref[...] += part

    @pl.when(pl.program_id(0) == pl.num_programs(0) - 1)
    def _():
        route_ref[...] = jnp.broadcast_to(acc_ref[...], route_ref.shape).astype(jnp.bfloat16)


def back(got, w_down, hidden, gate, up, block=256):
    parts, capacity, width = got.shape
    slots = parts * capacity
    hidden_width = w_down.shape[0]
    column = pl.BlockSpec((slots, block), lambda j: (0, j))
    return pl.pallas_call(
        back_kernel,
        grid=(hidden_width // block,),
        in_specs=[
            pl.BlockSpec(got.shape, lambda j: (0, 0, 0)),
            pl.BlockSpec((block, width), lambda j: (j, 0)),
            column,
            column,
            column,
        ],
        out_specs=[
            pl.BlockSpec((2, slots, block), lambda j: (0, 0, j)),
            pl.BlockSpec((slots, 128), lambda j: (0, 0)),
        ],
        out_shape=[
            jax.ShapeDtypeStruct((2, slots, hidden_width), jnp.bfloat16),
            jax.ShapeDtypeStruct((slots, 128), jnp.bfloat16),
        ],
        scratch_shapes=[pltpu.VMEM((slots, 1), jnp.float32)],
        compiler_params=pltpu.CompilerParams(vmem_limit_bytes=VMEM),
        cost_estimate=pl.CostEstimate(
            flops=2 * slots * hidden_width * width,
            bytes_accessed=2 * hidden_width * width + 2 * slots * width + 10 * slots * hidden_width,
            transcendentals=0,
        ),
        name="back",
    )(got, w_down, hidden, gate, up)


def turn_kernel(_, keep_ref, give_ref, keep_out, give_out):
    parts, capacity, block = keep_ref.shape
    keep_out[0, 0] = keep_ref[...].reshape(parts * capacity, block).T
    give_out[0, 0] = give_ref[...].reshape(parts * capacity, block).T


def turn(place, got, rings):
    parts, capacity, width = got.shape
    slots = parts * capacity
    block = width // (4 * rings)

    def column(half, ring, place_ref, core):
        side = jnp.where(half == 0, 1 - place_ref[0], place_ref[0])
        return (0, 0, (side * 2 + core) * rings + ring)

    out = pl.BlockSpec((1, 1, block, slots), lambda half, ring, _: (half, ring, 0, 0))
    return pl.pallas_call(
        turn_kernel,
        grid_spec=pltpu.PrefetchScalarGridSpec(
            num_scalar_prefetch=1,
            grid=(2, rings),
            in_specs=[
                pl.BlockSpec(
                    (parts, capacity, block), lambda half, ring, at: column(half, ring, at, at[1])
                ),
                pl.BlockSpec(
                    (parts, capacity, block), lambda half, ring, at: column(half, ring, at, 1 - at[1])
                ),
            ],
            out_specs=[out, out],
        ),
        out_shape=[jax.ShapeDtypeStruct((2, rings, block, slots), jnp.bfloat16)] * 2,
        compiler_params=pltpu.CompilerParams(vmem_limit_bytes=VMEM),
        cost_estimate=pl.CostEstimate(
            flops=slots * width * 1024, bytes_accessed=4 * slots * width, transcendentals=0
        ),
        name="turn",
    )(place, got, got)


def grad_in_kernel(keep_ref, came_ref, mine_ref, theirs_ref, out_ref):
    keep, came = keep_ref[0, 0], came_ref[0, 0]
    width = mine_ref.shape[2]
    for u in range(2):
        rows = contract(keep, mine_ref[u], 1, 0) + contract(came, theirs_ref[u], 1, 0)
        out_ref[0, 0, :, u * width : (u + 1) * width] = rows.astype(jnp.bfloat16)


def grad_down_kernel(keep_ref, came_ref, mine_ref, theirs_ref, far_out, near_out):
    rows = contract(keep_ref[0, 0], mine_ref[...], 1, 0) + contract(
        came_ref[0, 0], theirs_ref[...], 1, 0
    )
    rows = rows.astype(jnp.bfloat16)

    @pl.when(pl.program_id(0) == 0)
    def _():
        far_out[0] = rows

    @pl.when(pl.program_id(0) == 1)
    def _():
        near_out[0] = rows


def weight_grads(kernel, keep, came, mine, theirs, out_specs, out_shape):
    _, rings, block, slots = keep.shape
    left = pl.BlockSpec((1, 1, block, slots), lambda half, ring: (half, ring, 0, 0))
    whole = pl.BlockSpec(mine.shape, lambda half, ring: (0,) * mine.ndim)
    return pl.pallas_call(
        kernel,
        grid=(2, rings),
        in_specs=[left, left, whole, whole],
        out_specs=out_specs,
        out_shape=out_shape,
        compiler_params=pltpu.CompilerParams(vmem_limit_bytes=58 * 2**20),
        cost_estimate=pl.CostEstimate(
            flops=8 * rings * block * mine.size,
            bytes_accessed=8 * keep.size + 4 * mine.size + 4 * rings * block * mine.size // slots,
            transcendentals=0,
        ),
    )(keep, came, mine, theirs)


def slot_kernel(grads_ref, w_ref, out_ref):
    width = grads_ref.shape[2]
    rows = contract(grads_ref[0], w_ref[:, :width], 1, 1) + contract(
        grads_ref[1], w_ref[:, width:], 1, 1
    )
    out_ref[...] = rows.astype(jnp.bfloat16).reshape(out_ref.shape)


def slot_rows(grads, w_in, parts, block=512):
    _, slots, hidden_width = grads.shape
    width = w_in.shape[0]
    return pl.pallas_call(
        slot_kernel,
        grid=(width // block,),
        in_specs=[
            pl.BlockSpec(grads.shape, lambda j: (0, 0, 0)),
            pl.BlockSpec((block, 2 * hidden_width), lambda j: (j, 0)),
        ],
        out_specs=pl.BlockSpec((parts, slots // parts, block), lambda j: (0, 0, j)),
        out_shape=jax.ShapeDtypeStruct((parts, slots // parts, width), jnp.bfloat16),
        compiler_params=pltpu.CompilerParams(vmem_limit_bytes=VMEM),
        cost_estimate=pl.CostEstimate(
            flops=4 * slots * hidden_width * width,
            bytes_accessed=4 * hidden_width * width + 2 * slots * width,
            transcendentals=0,
        ),
        name="slot_rows",
    )(grads, w_in)


def exchange(rows):
    experts = lax.axis_size("expert")
    groups = [[(g ^ (e & 1)) * experts + e for e in range(experts)] for g in range(2)]
    return lax.all_to_all(
        rows,
        ("dp_0", "expert"),
        split_axis=0,
        concat_axis=0,
        axis_index_groups=groups,
        tiled=True,
    )


def per_device(residual, norm_gain, grad_out, expert_ids, route_weights, weight_in, weight_down):
    tok_rows, width = residual.shape
    topk = expert_ids.shape[1]
    hidden_width = weight_down.shape[1]
    experts = lax.axis_size("expert")
    capacity = min(tok_rows, 3 * tok_rows * topk // (2 * experts))
    slot_total = experts * capacity
    rings = lax.axis_size("ulysses")
    block = width // (4 * rings)
    side = lax.axis_index("dp_0")
    core = lax.axis_index("dp_1")
    ids_t = expert_ids.T
    weights_t = route_weights.T
    place, residual = lax.optimization_barrier(
        (jnp.stack([side, core]).astype(jnp.int32), residual)
    )

    send_normed, send_scaled, select = pack(
        ids_t, weights_t, norm_gain[None], residual, grad_out, experts, capacity
    )
    got_normed = exchange(send_normed)
    (got_normed, place, ids_t, weights_t, residual, grad_out, norm_gain, weight_in, weight_down) = (
        lax.optimization_barrier(
            (got_normed, place, ids_t, weights_t, residual, grad_out, norm_gain, weight_in, weight_down)
        )
    )
    got_scaled = exchange(send_scaled)
    w_in = weight_in[0]
    w_down = weight_down[0]
    keep_normed, give_normed = turn(place, got_normed, rings)
    came_normed = lax.ppermute(give_normed, "dp_1", SWAP)
    hidden, gate, up = forward(got_normed, w_in)
    their_hidden = lax.ppermute(hidden, "dp_1", SWAP)
    mine, route = back(got_scaled, w_down, hidden, gate, up)
    theirs = lax.ppermute(mine, "dp_1", SWAP)
    part_in = weight_grads(
        grad_in_kernel,
        keep_normed,
        came_normed,
        mine,
        theirs,
        pl.BlockSpec((1, 1, block, 2 * hidden_width), lambda half, ring: (ring, half, 0, 0)),
        jax.ShapeDtypeStruct((rings, 2, block, 2 * hidden_width), jnp.bfloat16),
    )
    keep_scaled, give_scaled = turn(place, got_scaled, rings)
    came_scaled = lax.ppermute(give_scaled, "dp_1", SWAP)
    far_down, near_down = weight_grads(
        grad_down_kernel,
        keep_scaled,
        came_scaled,
        hidden,
        their_hidden,
        [
            pl.BlockSpec(
                (1, block, hidden_width),
                lambda half, ring: (jnp.where(half == 0, ring, rings - 1), 0, 0),
            ),
            pl.BlockSpec(
                (1, block, hidden_width), lambda half, ring: (jnp.where(half == 0, 0, ring), 0, 0)
            ),
        ],
        [jax.ShapeDtypeStruct((rings, block, hidden_width), jnp.bfloat16)] * 2,
    )
    came_down = lax.ppermute(far_down, "dp_0", SWAP)
    summed_in = lax.psum_scatter(
        part_in.reshape(rings, 2 * block, 2 * hidden_width),
        "ulysses",
        scatter_dimension=0,
        tiled=True,
    )[0]
    came_in = lax.ppermute(summed_in[:block], "dp_0", SWAP)
    grad_in = (summed_in[block:].astype(jnp.float32) + came_in.astype(jnp.float32))[None]
    part_down = (near_down.astype(jnp.float32) + came_down.astype(jnp.float32)).astype(jnp.bfloat16)
    summed_down = lax.psum_scatter(part_down, "ulysses", scatter_dimension=0, tiled=True)
    summed_down, grad_in = lax.optimization_barrier((summed_down, grad_in))
    grad_down = summed_down.astype(jnp.float32)

    back_normed = exchange(slot_rows(mine, w_in, experts))
    back_route = exchange(route[:, 0].reshape(experts, capacity))
    resid = residual.astype(jnp.float32)
    inv_rms = lax.rsqrt(jnp.mean(resid * resid, axis=-1, keepdims=True) + eps)
    unit_rows = resid * inv_rms
    grad_normed = contract(select, back_normed.reshape(slot_total, width), 0, 0)
    token_route = jnp.sum(
        select.reshape(experts, capacity, tok_rows).astype(jnp.float32)
        * back_route.astype(jnp.float32)[:, :, None],
        axis=1,
    )
    chosen = ids_t[:, None, :] == lax.broadcasted_iota(jnp.int32, (1, experts, tok_rows), 1)
    route_t = jnp.sum(jnp.where(chosen, token_route[None], 0.0), axis=1)
    route_grad = (route_t / weights_t.astype(jnp.float32)).astype(jnp.bfloat16).T
    scaled_normed = grad_normed * norm_gain
    branch = inv_rms * (
        scaled_normed - unit_rows * jnp.mean(scaled_normed * unit_rows, axis=-1, keepdims=True)
    )
    grad_residual = (grad_out.astype(jnp.float32) + branch).astype(jnp.bfloat16)
    return (grad_residual, route_grad, grad_in, grad_down)


def solution(mesh):
    finer = Mesh(
        mesh.devices.reshape(2, 2, mesh.shape["ulysses"], mesh.shape["expert"]),
        ("dp_0", "dp_1", "ulysses", "expert"),
    )
    return jax.shard_map(
        per_device,
        mesh=finer,
        in_specs=(
            P(DP_ULYSSES_EXPERT, None),
            P(),
            P(DP_ULYSSES_EXPERT, None),
            P(DP_ULYSSES_EXPERT, None),
            P(DP_ULYSSES_EXPERT, None),
            P("expert", None, None),
            P("expert", None, None),
        ),
        out_specs=(
            P(DP_ULYSSES_EXPERT, None),
            P(DP_ULYSSES_EXPERT, None),
            P("expert", DP_ULYSSES, None),
            P("expert", DP_ULYSSES, None),
        ),
        check_vma=False,
    )
```

```python
import jax
import jax.numpy as jnp
from jax import lax
from jax.experimental import pallas as pl
from jax.experimental.pallas import tpu as pltpu
from jax.sharding import Mesh
from jax.sharding import PartitionSpec as P

DP_ULYSSES = ("dp_0", "dp_1", "ulysses")
DP_ULYSSES_EXPERT = ("dp_0", "dp_1", "ulysses", "expert")

SWAP = [(0, 1), (1, 0)]

eps = 1e-06

VMEM = 62 * 2**20


def contract(left, right, over_left, over_right):
    return lax.dot_general(
        left, right, (((over_left,), (over_right,)), ((), ())), preferred_element_type=jnp.float32
    )


def slot_matrices(ids, weights, experts, capacity):
    tok_rows = ids.shape[1]
    expert = lax.broadcasted_iota(jnp.int32, (experts, tok_rows), 0)
    first, second = ids[0:1] == expert, ids[1:2] == expert
    hit = first | second
    weight = jnp.where(first, weights[0:1], jnp.where(second, weights[1:2], 0.0))
    square = (tok_rows, tok_rows)
    before = lax.broadcasted_iota(jnp.int32, square, 0) < lax.broadcasted_iota(jnp.int32, square, 1)
    rank = contract(
        jnp.where(hit, 1.0, 0.0).astype(jnp.bfloat16),
        jnp.where(before, 1.0, 0.0).astype(jnp.bfloat16),
        1,
        0,
    ).astype(jnp.int32)
    rank = jnp.where(hit, rank, capacity)
    slot = lax.broadcasted_iota(jnp.int32, (capacity, tok_rows), 0)
    select, scale = [], []
    for e in range(experts):
        held = rank[e : e + 1] == slot
        select.append(jnp.where(held, 1.0, 0.0))
        scale.append(jnp.where(held, weight[e : e + 1], 0.0))
    return (
        jnp.concatenate(select, axis=0).astype(jnp.bfloat16),
        jnp.concatenate(scale, axis=0).astype(jnp.bfloat16),
    )


def pack_kernel(
    ids_ref, w_ref, gain_ref, resid_ref, grad_ref, normed_ref, scaled_ref, sel_ref, inv_ref, scale_ref
):
    experts, capacity, block = normed_ref.shape

    @pl.when(pl.program_id(0) == 0)
    def _():
        full = resid_ref[...].astype(jnp.float32)
        mean = jnp.mean(full * full, axis=-1, keepdims=True)
        inv_ref[...] = lax.rsqrt(mean + eps)
        select, scale = slot_matrices(ids_ref[...], w_ref[...].astype(jnp.float32), experts, capacity)
        sel_ref[...] = select
        scale_ref[...] = scale

    at = pl.ds(pl.multiple_of(pl.program_id(0) * block, block), block)
    unit = resid_ref[:, at].astype(jnp.float32) * inv_ref[...]
    normed = (unit * gain_ref[:, at]).astype(jnp.bfloat16)
    sent = contract(sel_ref[...], normed, 1, 0).astype(jnp.bfloat16)
    normed_ref[...] = sent.reshape(experts, capacity, block)
    sent = contract(scale_ref[...], grad_ref[:, at], 1, 0).astype(jnp.bfloat16)
    scaled_ref[...] = sent.reshape(experts, capacity, block)


def pack(ids_t, w_t, gain, resid, grad, experts, capacity, block=1024):
    rows, width = resid.shape
    whole = lambda a: pl.BlockSpec(a.shape, lambda j: (0,) * a.ndim)
    args = (ids_t, w_t, gain, resid, grad)
    slots = experts * capacity
    return pl.pallas_call(
        pack_kernel,
        grid=(width // block,),
        in_specs=[whole(a) for a in args],
        out_specs=[
            pl.BlockSpec((experts, capacity, block), lambda j: (0, 0, j)),
            pl.BlockSpec((experts, capacity, block), lambda j: (0, 0, j)),
            pl.BlockSpec((slots, rows), lambda j: (0, 0)),
        ],
        out_shape=[
            jax.ShapeDtypeStruct((experts, capacity, width), jnp.bfloat16),
            jax.ShapeDtypeStruct((experts, capacity, width), jnp.bfloat16),
            jax.ShapeDtypeStruct((slots, rows), jnp.bfloat16),
        ],
        scratch_shapes=[
            pltpu.VMEM((rows, 1), jnp.float32),
            pltpu.VMEM((slots, rows), jnp.bfloat16),
        ],
        compiler_params=pltpu.CompilerParams(vmem_limit_bytes=VMEM),
        cost_estimate=pl.CostEstimate(
            flops=4 * slots * rows * width, bytes_accessed=4 * slots * width, transcendentals=0
        ),
        name="pack",
    )(*args)


def forward_kernel(got_ref, gate_w_ref, up_w_ref, hidden_ref, gate_ref, up_ref):
    parts, capacity, width = got_ref.shape
    normed = got_ref[...].reshape(parts * capacity, width)
    gate = contract(normed, gate_w_ref[...], 1, 0)
    up = contract(normed, up_w_ref[...], 1, 0)
    sigmoid = jax.nn.sigmoid(gate)
    silu = gate * sigmoid
    hidden_ref[...] = (silu * up).astype(jnp.bfloat16)
    gate_ref[...] = up * sigmoid * (1.0 + gate * (1.0 - sigmoid))
    up_ref[...] = silu


def forward(got, w_in, block=256):
    parts, capacity, width = got.shape
    slots = parts * capacity
    hidden_width = w_in.shape[1] // 2
    steps = hidden_width // block
    out = pl.BlockSpec((slots, block), lambda j: (0, j))
    return pl.pallas_call(
        forward_kernel,
        grid=(steps,),
        in_specs=[
            pl.BlockSpec(got.shape, lambda j: (0, 0, 0)),
            pl.BlockSpec((width, block), lambda j: (0, j)),
            pl.BlockSpec((width, block), lambda j: (0, steps + j)),
        ],
        out_specs=[out] * 3,
        out_shape=[
            jax.ShapeDtypeStruct((slots, hidden_width), t)
            for t in (jnp.bfloat16, jnp.float32, jnp.float32)
        ],
        compiler_params=pltpu.CompilerParams(vmem_limit_bytes=VMEM),
        cost_estimate=pl.CostEstimate(
            flops=4 * slots * hidden_width * width,
            bytes_accessed=4 * hidden_width * width + 2 * slots * width,
            transcendentals=slots * hidden_width,
        ),
        name="forward",
    )(got, w_in, w_in)


def back_kernel(got_ref, w_ref, hidden_ref, gate_ref, up_ref, out_ref, route_ref, acc_ref):
    parts, capacity, width = got_ref.shape
    grad_hidden = contract(got_ref[...].reshape(parts * capacity, width), w_ref[...], 1, 1)
    out_ref[0] = (grad_hidden * gate_ref[...]).astype(jnp.bfloat16)
    out_ref[1] = (grad_hidden * up_ref[...]).astype(jnp.bfloat16)
    part = jnp.sum(grad_hidden * hidden_ref[...].astype(jnp.float32), axis=1, keepdims=True)

    @pl.when(pl.program_id(0) == 0)
    def _():
        acc_ref[...] = part

    @pl.when(pl.program_id(0) > 0)
    def _():
        acc_ref[...] += part

    @pl.when(pl.program_id(0) == pl.num_programs(0) - 1)
    def _():
        route_ref[...] = jnp.broadcast_to(acc_ref[...], route_ref.shape).astype(jnp.bfloat16)


def back(got, w_down, hidden, gate, up, block=256):
    parts, capacity, width = got.shape
    slots = parts * capacity
    hidden_width = w_down.shape[0]
    column = pl.BlockSpec((slots, block), lambda j: (0, j))
    return pl.pallas_call(
        back_kernel,
        grid=(hidden_width // block,),
        in_specs=[
            pl.BlockSpec(got.shape, lambda j: (0, 0, 0)),
            pl.BlockSpec((block, width), lambda j: (j, 0)),
            column,
            column,
            column,
        ],
        out_specs=[
            pl.BlockSpec((2, slots, block), lambda j: (0, 0, j)),
            pl.BlockSpec((slots, 128), lambda j: (0, 0)),
        ],
        out_shape=[
            jax.ShapeDtypeStruct((2, slots, hidden_width), jnp.bfloat16),
            jax.ShapeDtypeStruct((slots, 128), jnp.bfloat16),
        ],
        scratch_shapes=[pltpu.VMEM((slots, 1), jnp.float32)],
        compiler_params=pltpu.CompilerParams(vmem_limit_bytes=VMEM),
        cost_estimate=pl.CostEstimate(
            flops=2 * slots * hidden_width * width,
            bytes_accessed=2 * hidden_width * width + 2 * slots * width + 10 * slots * hidden_width,
            transcendentals=0,
        ),
        name="back",
    )(got, w_down, hidden, gate, up)


def turn_kernel(_, keep_ref, give_ref, keep_out, give_out):
    parts, capacity, block = keep_ref.shape
    keep_out[0] = keep_ref[...].reshape(parts * capacity, block).T.reshape(keep_out.shape[1:])
    give_out[0] = give_ref[...].reshape(parts * capacity, block).T.reshape(give_out.shape[1:])


def turn(place, got, rings, span):
    parts, capacity, width = got.shape
    slots = parts * capacity
    block = width // (4 * rings)
    steps = rings // span

    def column(half, ring, place_ref, core):
        side = jnp.where(half == 0, 1 - place_ref[0], place_ref[0])
        return (0, 0, (side * 2 + core) * steps + ring)

    out = pl.BlockSpec((1, span, block, slots), lambda half, ring, _: (half, ring, 0, 0))
    return pl.pallas_call(
        turn_kernel,
        grid_spec=pltpu.PrefetchScalarGridSpec(
            num_scalar_prefetch=1,
            grid=(2, steps),
            in_specs=[
                pl.BlockSpec(
                    (parts, capacity, span * block),
                    lambda half, ring, at: column(half, ring, at, at[1]),
                ),
                pl.BlockSpec(
                    (parts, capacity, span * block),
                    lambda half, ring, at: column(half, ring, at, 1 - at[1]),
                ),
            ],
            out_specs=[out, out],
        ),
        out_shape=[jax.ShapeDtypeStruct((2, rings, block, slots), jnp.bfloat16)] * 2,
        compiler_params=pltpu.CompilerParams(vmem_limit_bytes=VMEM),
        cost_estimate=pl.CostEstimate(
            flops=slots * width * 1024, bytes_accessed=4 * slots * width, transcendentals=0
        ),
        name="turn",
    )(place, got, got)


def both_cores(keep_ref, came_ref):
    span, block, slots = keep_ref.shape[1:]
    both = (keep_ref[0].reshape(span * block, slots), came_ref[0].reshape(span * block, slots))
    return jnp.concatenate(both, axis=1)


def grad_in_kernel(keep_ref, came_ref, mine_ref, theirs_ref, out_ref, right_ref):
    span, _, block, _ = out_ref.shape
    _, slots, width = mine_ref.shape

    @pl.when((pl.program_id(0) == 0) & (pl.program_id(1) == 0))
    def _():
        for u in range(2):
            right_ref[:slots, u * width : (u + 1) * width] = mine_ref[u]
            right_ref[slots:, u * width : (u + 1) * width] = theirs_ref[u]

    rows = contract(both_cores(keep_ref, came_ref), right_ref[...], 1, 0).astype(jnp.bfloat16)
    out_ref[:, 0] = rows.reshape(span, block, 2 * width)


def grad_down_kernel(keep_ref, came_ref, mine_ref, theirs_ref, far_out, near_out, right_ref):
    slots = mine_ref.shape[0]

    @pl.when((pl.program_id(0) == 0) & (pl.program_id(1) == 0))
    def _():
        right_ref[:slots] = mine_ref[...]
        right_ref[slots:] = theirs_ref[...]

    rows = contract(both_cores(keep_ref, came_ref), right_ref[...], 1, 0).astype(jnp.bfloat16)

    @pl.when(pl.program_id(0) == 0)
    def _():
        far_out[...] = rows.reshape(far_out.shape)

    @pl.when(pl.program_id(0) == 1)
    def _():
        near_out[...] = rows.reshape(near_out.shape)


def weight_grads(kernel, keep, came, mine, theirs, span, out_specs, out_shape):
    _, rings, block, slots = keep.shape
    left = pl.BlockSpec((1, span, block, slots), lambda half, ring: (half, ring, 0, 0))
    whole = pl.BlockSpec(mine.shape, lambda half, ring: (0,) * mine.ndim)
    return pl.pallas_call(
        kernel,
        grid=(2, rings // span),
        in_specs=[left, left, whole, whole],
        out_specs=out_specs,
        out_shape=out_shape,
        scratch_shapes=[pltpu.VMEM((2 * slots, mine.size // slots), jnp.bfloat16)],
        compiler_params=pltpu.CompilerParams(vmem_limit_bytes=58 * 2**20),
        cost_estimate=pl.CostEstimate(
            flops=8 * rings * block * mine.size,
            bytes_accessed=8 * keep.size + 4 * mine.size + 4 * rings * block * mine.size // slots,
            transcendentals=0,
        ),
    )(keep, came, mine, theirs)


def slot_kernel(grads_ref, w_ref, out_ref):
    width = grads_ref.shape[2]
    rows = contract(grads_ref[0], w_ref[:, :width], 1, 1) + contract(
        grads_ref[1], w_ref[:, width:], 1, 1
    )
    out_ref[...] = rows.astype(jnp.bfloat16).reshape(out_ref.shape)


def slot_rows(grads, w_in, parts, block=1024):
    _, slots, hidden_width = grads.shape
    width = w_in.shape[0]
    return pl.pallas_call(
        slot_kernel,
        grid=(width // block,),
        in_specs=[
            pl.BlockSpec(grads.shape, lambda j: (0, 0, 0)),
            pl.BlockSpec((block, 2 * hidden_width), lambda j: (j, 0)),
        ],
        out_specs=pl.BlockSpec((parts, slots // parts, block), lambda j: (0, 0, j)),
        out_shape=jax.ShapeDtypeStruct((parts, slots // parts, width), jnp.bfloat16),
        compiler_params=pltpu.CompilerParams(vmem_limit_bytes=VMEM),
        cost_estimate=pl.CostEstimate(
            flops=4 * slots * hidden_width * width,
            bytes_accessed=4 * hidden_width * width + 2 * slots * width,
            transcendentals=0,
        ),
        name="slot_rows",
    )(grads, w_in)


def exchange(rows):
    experts = lax.axis_size("expert")
    groups = [[(g ^ (e & 1)) * experts + e for e in range(experts)] for g in range(2)]
    return lax.all_to_all(
        rows,
        ("dp_0", "expert"),
        split_axis=0,
        concat_axis=0,
        axis_index_groups=groups,
        tiled=True,
    )


def per_device(residual, norm_gain, grad_out, expert_ids, route_weights, weight_in, weight_down):
    tok_rows, width = residual.shape
    topk = expert_ids.shape[1]
    hidden_width = weight_down.shape[1]
    experts = lax.axis_size("expert")
    capacity = min(tok_rows, 3 * tok_rows * topk // (2 * experts))
    slot_total = experts * capacity
    rings = lax.axis_size("ulysses")
    block = width // (4 * rings)
    span = 2 if rings % 2 == 0 else 1
    side = lax.axis_index("dp_0")
    core = lax.axis_index("dp_1")
    ids_t = expert_ids.T
    weights_t = route_weights.T
    place, residual = lax.optimization_barrier(
        (jnp.stack([side, core]).astype(jnp.int32), residual)
    )

    send_normed, send_scaled, select = pack(
        ids_t, weights_t, norm_gain[None], residual, grad_out, experts, capacity
    )
    got_normed = exchange(send_normed)
    (got_normed, place, ids_t, weights_t, residual, grad_out, norm_gain, weight_in, weight_down) = (
        lax.optimization_barrier(
            (got_normed, place, ids_t, weights_t, residual, grad_out, norm_gain, weight_in, weight_down)
        )
    )
    got_scaled = exchange(send_scaled)
    w_in = weight_in[0]
    w_down = weight_down[0]
    keep_normed, give_normed = turn(place, got_normed, rings, span)
    came_normed = lax.ppermute(give_normed, "dp_1", SWAP)
    hidden, gate, up = forward(got_normed, w_in)
    their_hidden = lax.ppermute(hidden, "dp_1", SWAP)
    mine, route = back(got_scaled, w_down, hidden, gate, up)
    theirs = lax.ppermute(mine, "dp_1", SWAP)
    part_in = weight_grads(
        grad_in_kernel,
        keep_normed,
        came_normed,
        mine,
        theirs,
        span,
        pl.BlockSpec((span, 1, block, 2 * hidden_width), lambda half, ring: (ring, half, 0, 0)),
        jax.ShapeDtypeStruct((rings, 2, block, 2 * hidden_width), jnp.bfloat16),
    )
    keep_scaled, give_scaled = turn(place, got_scaled, rings, span)
    came_scaled = lax.ppermute(give_scaled, "dp_1", SWAP)
    far_down, near_down = weight_grads(
        grad_down_kernel,
        keep_scaled,
        came_scaled,
        hidden,
        their_hidden,
        span,
        [
            pl.BlockSpec(
                (span, block, hidden_width),
                lambda half, ring: (jnp.where(half == 0, ring, rings // span - 1), 0, 0),
            ),
            pl.BlockSpec(
                (span, block, hidden_width),
                lambda half, ring: (jnp.where(half == 0, 0, ring), 0, 0),
            ),
        ],
        [jax.ShapeDtypeStruct((rings, block, hidden_width), jnp.bfloat16)] * 2,
    )
    came_down = lax.ppermute(far_down, "dp_0", SWAP)
    summed_in = lax.psum_scatter(
        part_in.reshape(rings, 2 * block, 2 * hidden_width),
        "ulysses",
        scatter_dimension=0,
        tiled=True,
    )[0]
    came_in = lax.ppermute(summed_in[:block], "dp_0", SWAP)
    grad_in = (summed_in[block:].astype(jnp.float32) + came_in.astype(jnp.float32))[None]
    part_down = (near_down.astype(jnp.float32) + came_down.astype(jnp.float32)).astype(jnp.bfloat16)
    summed_down = lax.psum_scatter(part_down, "ulysses", scatter_dimension=0, tiled=True)
    summed_down, grad_in = lax.optimization_barrier((summed_down, grad_in))
    grad_down = summed_down.astype(jnp.float32)

    mine, route, far_down = lax.optimization_barrier((mine, route, far_down))
    slot_normed = slot_rows(mine, w_in, experts)
    back_normed = exchange(slot_normed)
    back_route = exchange(route[:, 0].reshape(experts, capacity))
    resid = residual.astype(jnp.float32)
    inv_rms = lax.rsqrt(jnp.mean(resid * resid, axis=-1, keepdims=True) + eps)
    unit_rows = resid * inv_rms
    grad_normed = contract(select, back_normed.reshape(slot_total, width), 0, 0)
    token_route = jnp.sum(
        select.reshape(experts, capacity, tok_rows).astype(jnp.float32)
        * back_route.astype(jnp.float32)[:, :, None],
        axis=1,
    )
    chosen = ids_t[:, None, :] == lax.broadcasted_iota(jnp.int32, (1, experts, tok_rows), 1)
    route_t = jnp.sum(jnp.where(chosen, token_route[None], 0.0), axis=1)
    route_grad = (route_t / weights_t.astype(jnp.float32)).astype(jnp.bfloat16).T
    scaled_normed = grad_normed * norm_gain
    branch = inv_rms * (
        scaled_normed - unit_rows * jnp.mean(scaled_normed * unit_rows, axis=-1, keepdims=True)
    )
    grad_residual = (grad_out.astype(jnp.float32) + branch).astype(jnp.bfloat16)
    return (grad_residual, route_grad, grad_in, grad_down)


def solution(mesh):
    finer = Mesh(
        mesh.devices.reshape(2, 2, mesh.shape["ulysses"], mesh.shape["expert"]),
        ("dp_0", "dp_1", "ulysses", "expert"),
    )
    return jax.shard_map(
        per_device,
        mesh=finer,
        in_specs=(
            P(DP_ULYSSES_EXPERT, None),
            P(),
            P(DP_ULYSSES_EXPERT, None),
            P(DP_ULYSSES_EXPERT, None),
            P(DP_ULYSSES_EXPERT, None),
            P("expert", None, None),
            P("expert", None, None),
        ),
        out_specs=(
            P(DP_ULYSSES_EXPERT, None),
            P(DP_ULYSSES_EXPERT, None),
            P("expert", DP_ULYSSES, None),
            P("expert", DP_ULYSSES, None),
        ),
        check_vma=False,
    )
```

```python
import jax
import jax.numpy as jnp
from jax import lax
from jax.experimental import pallas as pl
from jax.experimental.pallas import tpu as pltpu
from jax.sharding import Mesh
from jax.sharding import PartitionSpec as P


DP_ULYSSES = ("dp_0", "dp_1", "ulysses")
DP_ULYSSES_EXPERT = ("dp_0", "dp_1", "ulysses", "expert")

SWAP = [(0, 1), (1, 0)]

eps = 1e-06

VMEM = 62 * 2**20


def contract(left, right, over_left, over_right):
    return lax.dot_general(
        left, right, (((over_left,), (over_right,)), ((), ())), preferred_element_type=jnp.float32
    )


def slot_matrices(ids, weights, experts, capacity):
    tok_rows = ids.shape[1]
    expert = lax.broadcasted_iota(jnp.int32, (experts, tok_rows), 0)
    first, second = ids[0:1] == expert, ids[1:2] == expert
    hit = first | second
    weight = jnp.where(first, weights[0:1], jnp.where(second, weights[1:2], 0.0))
    square = (tok_rows, tok_rows)
    before = lax.broadcasted_iota(jnp.int32, square, 0) < lax.broadcasted_iota(jnp.int32, square, 1)
    rank = contract(
        jnp.where(hit, 1.0, 0.0).astype(jnp.bfloat16),
        jnp.where(before, 1.0, 0.0).astype(jnp.bfloat16),
        1,
        0,
    ).astype(jnp.int32)
    rank = jnp.where(hit, rank, capacity)
    slot = lax.broadcasted_iota(jnp.int32, (capacity, tok_rows), 0)
    select, scale = [], []
    for e in range(experts):
        held = rank[e : e + 1] == slot
        select.append(jnp.where(held, 1.0, 0.0))
        scale.append(jnp.where(held, weight[e : e + 1], 0.0))
    return (
        jnp.concatenate(select, axis=0).astype(jnp.bfloat16),
        jnp.concatenate(scale, axis=0).astype(jnp.bfloat16),
    )


def pack_kernel(
    ids_ref, w_ref, gain_ref, resid_ref, grad_ref, normed_ref, scaled_ref, sel_ref, inv_ref, scale_ref
):
    experts, capacity, block = normed_ref.shape

    @pl.when(pl.program_id(0) == 0)
    def _():
        full = resid_ref[...].astype(jnp.float32)
        mean = jnp.mean(full * full, axis=-1, keepdims=True)
        inv_ref[...] = lax.rsqrt(mean + eps)
        select, scale = slot_matrices(ids_ref[...], w_ref[...].astype(jnp.float32), experts, capacity)
        sel_ref[...] = select
        scale_ref[...] = scale

    at = pl.ds(pl.multiple_of(pl.program_id(0) * block, block), block)
    unit = resid_ref[:, at].astype(jnp.float32) * inv_ref[...]
    normed = (unit * gain_ref[:, at]).astype(jnp.bfloat16)
    sent = contract(sel_ref[...], normed, 1, 0).astype(jnp.bfloat16)
    normed_ref[...] = sent.reshape(experts, capacity, block)
    sent = contract(scale_ref[...], grad_ref[:, at], 1, 0).astype(jnp.bfloat16)
    scaled_ref[...] = sent.reshape(experts, capacity, block)


def pack(ids_t, w_t, gain, resid, grad, experts, capacity, block=1024):
    rows, width = resid.shape
    whole = lambda a: pl.BlockSpec(a.shape, lambda j: (0,) * a.ndim)
    args = (ids_t, w_t, gain, resid, grad)
    slots = experts * capacity
    return pl.pallas_call(
        pack_kernel,
        grid=(width // block,),
        in_specs=[whole(a) for a in args],
        out_specs=[
            pl.BlockSpec((experts, capacity, block), lambda j: (0, 0, j)),
            pl.BlockSpec((experts, capacity, block), lambda j: (0, 0, j)),
            pl.BlockSpec((slots, rows), lambda j: (0, 0)),
        ],
        out_shape=[
            jax.ShapeDtypeStruct((experts, capacity, width), jnp.bfloat16),
            jax.ShapeDtypeStruct((experts, capacity, width), jnp.bfloat16),
            jax.ShapeDtypeStruct((slots, rows), jnp.bfloat16),
        ],
        scratch_shapes=[
            pltpu.VMEM((rows, 1), jnp.float32),
            pltpu.VMEM((slots, rows), jnp.bfloat16),
        ],
        compiler_params=pltpu.CompilerParams(vmem_limit_bytes=VMEM),
        cost_estimate=pl.CostEstimate(
            flops=4 * slots * rows * width, bytes_accessed=4 * slots * width, transcendentals=0
        ),
        name="pack",
    )(*args)


def forward_kernel(got_ref, gate_w_ref, up_w_ref, hidden_ref, gate_ref, up_ref):
    parts, capacity, width = got_ref.shape
    normed = got_ref[...].reshape(parts * capacity, width)
    gate = contract(normed, gate_w_ref[...], 1, 0)
    up = contract(normed, up_w_ref[...], 1, 0)
    sigmoid = jax.nn.sigmoid(gate)
    silu = gate * sigmoid
    hidden_ref[...] = (silu * up).astype(jnp.bfloat16)
    gate_ref[...] = up * sigmoid * (1.0 + gate * (1.0 - sigmoid))
    up_ref[...] = silu


def forward(got, w_in, block=256):
    parts, capacity, width = got.shape
    slots = parts * capacity
    hidden_width = w_in.shape[1] // 2
    steps = hidden_width // block
    out = pl.BlockSpec((slots, block), lambda j: (0, j))
    return pl.pallas_call(
        forward_kernel,
        grid=(steps,),
        in_specs=[
            pl.BlockSpec(got.shape, lambda j: (0, 0, 0)),
            pl.BlockSpec((width, block), lambda j: (0, j)),
            pl.BlockSpec((width, block), lambda j: (0, steps + j)),
        ],
        out_specs=[out] * 3,
        out_shape=[
            jax.ShapeDtypeStruct((slots, hidden_width), t)
            for t in (jnp.bfloat16, jnp.float32, jnp.float32)
        ],
        compiler_params=pltpu.CompilerParams(vmem_limit_bytes=VMEM),
        cost_estimate=pl.CostEstimate(
            flops=4 * slots * hidden_width * width,
            bytes_accessed=4 * hidden_width * width + 2 * slots * width,
            transcendentals=slots * hidden_width,
        ),
        name="forward",
    )(got, w_in, w_in)


def back_kernel(got_ref, w_ref, hidden_ref, gate_ref, up_ref, out_ref, route_ref, acc_ref):
    parts, capacity, width = got_ref.shape
    grad_hidden = contract(got_ref[...].reshape(parts * capacity, width), w_ref[...], 1, 1)
    out_ref[0] = (grad_hidden * gate_ref[...]).astype(jnp.bfloat16)
    out_ref[1] = (grad_hidden * up_ref[...]).astype(jnp.bfloat16)
    part = jnp.sum(grad_hidden * hidden_ref[...].astype(jnp.float32), axis=1, keepdims=True)

    @pl.when(pl.program_id(0) == 0)
    def _():
        acc_ref[...] = part

    @pl.when(pl.program_id(0) > 0)
    def _():
        acc_ref[...] += part

    @pl.when(pl.program_id(0) == pl.num_programs(0) - 1)
    def _():
        route_ref[...] = jnp.broadcast_to(acc_ref[...], route_ref.shape).astype(jnp.bfloat16)


def back(got, w_down, hidden, gate, up, block=256):
    parts, capacity, width = got.shape
    slots = parts * capacity
    hidden_width = w_down.shape[0]
    column = pl.BlockSpec((slots, block), lambda j: (0, j))
    return pl.pallas_call(
        back_kernel,
        grid=(hidden_width // block,),
        in_specs=[
            pl.BlockSpec(got.shape, lambda j: (0, 0, 0)),
            pl.BlockSpec((block, width), lambda j: (j, 0)),
            column,
            column,
            column,
        ],
        out_specs=[
            pl.BlockSpec((2, slots, block), lambda j: (0, 0, j)),
            pl.BlockSpec((slots, 128), lambda j: (0, 0)),
        ],
        out_shape=[
            jax.ShapeDtypeStruct((2, slots, hidden_width), jnp.bfloat16),
            jax.ShapeDtypeStruct((slots, 128), jnp.bfloat16),
        ],
        scratch_shapes=[pltpu.VMEM((slots, 1), jnp.float32)],
        compiler_params=pltpu.CompilerParams(vmem_limit_bytes=VMEM),
        cost_estimate=pl.CostEstimate(
            flops=2 * slots * hidden_width * width,
            bytes_accessed=2 * hidden_width * width + 2 * slots * width + 10 * slots * hidden_width,
            transcendentals=0,
        ),
        name="back",
    )(got, w_down, hidden, gate, up)


def turn_kernel(_, keep_ref, give_ref, keep_out, give_out):
    parts, capacity, block = keep_ref.shape
    keep_out[0] = keep_ref[...].reshape(parts * capacity, block).T.reshape(keep_out.shape[1:])
    give_out[0] = give_ref[...].reshape(parts * capacity, block).T.reshape(give_out.shape[1:])


def turn(place, got, rings, span):
    parts, capacity, width = got.shape
    slots = parts * capacity
    block = width // (4 * rings)
    steps = rings // span

    def column(half, ring, place_ref, core):
        side = jnp.where(half == 0, 1 - place_ref[0], place_ref[0])
        return (0, 0, (side * 2 + core) * steps + ring)

    out = pl.BlockSpec((1, span, block, slots), lambda half, ring, _: (half, ring, 0, 0))
    return pl.pallas_call(
        turn_kernel,
        grid_spec=pltpu.PrefetchScalarGridSpec(
            num_scalar_prefetch=1,
            grid=(2, steps),
            in_specs=[
                pl.BlockSpec(
                    (parts, capacity, span * block),
                    lambda half, ring, at: column(half, ring, at, at[1]),
                ),
                pl.BlockSpec(
                    (parts, capacity, span * block),
                    lambda half, ring, at: column(half, ring, at, 1 - at[1]),
                ),
            ],
            out_specs=[out, out],
        ),
        out_shape=[jax.ShapeDtypeStruct((2, rings, block, slots), jnp.bfloat16)] * 2,
        compiler_params=pltpu.CompilerParams(vmem_limit_bytes=VMEM),
        cost_estimate=pl.CostEstimate(
            flops=slots * width * 1024, bytes_accessed=4 * slots * width, transcendentals=0
        ),
        name="turn",
    )(place, got, got)


def rows_kernel(_, keep_ref, came_ref, mine_ref, theirs_ref, far_ref, near_ref):
    block, slots = keep_ref.shape[2:]
    keep, came = keep_ref[...].reshape(2 * block, slots), came_ref[...].reshape(2 * block, slots)
    rows = contract(keep, mine_ref[0], 1, 0) + contract(came, theirs_ref[0], 1, 0)
    rows = rows.astype(jnp.bfloat16)
    far_ref[0] = rows[:block]
    near_ref[0] = rows[block:]


def weight_rows(place, keep, came, mine, theirs, first, count):
    _, rings, block, slots = keep.shape
    units, _, width = mine.shape
    left = pl.BlockSpec(
        (2, 1, block, slots), lambda i, u, at: (0, lax.rem(at[2] + (first + i), rings), 0, 0)
    )
    right = pl.BlockSpec((1, slots, width), lambda i, u, at: (u, 0, 0))
    out = pl.BlockSpec((1, block, width), lambda i, u, at: (i, 0, u))
    return pl.pallas_call(
        rows_kernel,
        grid_spec=pltpu.PrefetchScalarGridSpec(
            num_scalar_prefetch=1,
            grid=(count, units),
            in_specs=[left, left, right, right],
            out_specs=[out, out],
        ),
        out_shape=[jax.ShapeDtypeStruct((count, block, units * width), jnp.bfloat16)] * 2,
        compiler_params=pltpu.CompilerParams(vmem_limit_bytes=VMEM),
        cost_estimate=pl.CostEstimate(
            flops=8 * count * block * mine.size,
            bytes_accessed=4 * mine.size + 4 * count * block * (2 * slots + units * width),
            transcendentals=0,
        ),
    )(place, keep, came, mine, theirs)


def slot_kernel(grads_ref, w_ref, out_ref):
    width = grads_ref.shape[2]
    rows = contract(grads_ref[0], w_ref[:, :width], 1, 1) + contract(
        grads_ref[1], w_ref[:, width:], 1, 1
    )
    out_ref[...] = rows.astype(jnp.bfloat16).reshape(out_ref.shape)


def slot_rows(grads, w_in, parts, block=1024):
    _, slots, hidden_width = grads.shape
    width = w_in.shape[0]
    return pl.pallas_call(
        slot_kernel,
        grid=(width // block,),
        in_specs=[
            pl.BlockSpec(grads.shape, lambda j: (0, 0, 0)),
            pl.BlockSpec((block, 2 * hidden_width), lambda j: (j, 0)),
        ],
        out_specs=pl.BlockSpec((parts, slots // parts, block), lambda j: (0, 0, j)),
        out_shape=jax.ShapeDtypeStruct((parts, slots // parts, width), jnp.bfloat16),
        compiler_params=pltpu.CompilerParams(vmem_limit_bytes=VMEM),
        cost_estimate=pl.CostEstimate(
            flops=4 * slots * hidden_width * width,
            bytes_accessed=4 * hidden_width * width + 2 * slots * width,
            transcendentals=0,
        ),
        name="slot_rows",
    )(grads, w_in)


def added(*terms):
    return sum(t.astype(jnp.float32) for t in terms)


def ring_sum(low, high):
    size = lax.axis_size("ulysses")
    ahead = [(i, (i + 1) % size) for i in range(size)]
    behind = [(i, (i - 1) % size) for i in range(size)]
    low_two = lax.ppermute(low[2], "ulysses", ahead)
    high_two = lax.ppermute(high[2], "ulysses", behind)
    high_side = lax.ppermute(high[1], "ulysses", ahead)
    low_side = lax.ppermute(low[3], "ulysses", behind)
    low_both = added(low[1], low_two).astype(jnp.bfloat16)
    high_both = added(high[3], high_two).astype(jnp.bfloat16)
    low_last = lax.ppermute(low_both, "ulysses", ahead)
    high_last = lax.ppermute(high_both, "ulysses", behind)
    sums = added(low[0], low_last, low_side), added(high[0], high_last, high_side)
    return sums, low_both, high_both


def exchange(rows):
    experts = lax.axis_size("expert")
    groups = [[(g ^ (e & 1)) * experts + e for e in range(experts)] for g in range(2)]
    return lax.all_to_all(
        rows,
        ("dp_0", "expert"),
        split_axis=0,
        concat_axis=0,
        axis_index_groups=groups,
        tiled=True,
    )


def per_device(residual, norm_gain, grad_out, expert_ids, route_weights, weight_in, weight_down):
    tok_rows, width = residual.shape
    topk = expert_ids.shape[1]
    experts = lax.axis_size("expert")
    capacity = min(tok_rows, 3 * tok_rows * topk // (2 * experts))
    slot_total = experts * capacity
    rings = lax.axis_size("ulysses")
    block = width // (4 * rings)
    span = 2 if rings % 2 == 0 else 1
    side = lax.axis_index("dp_0")
    core = lax.axis_index("dp_1")
    ids_t = expert_ids.T
    weights_t = route_weights.T
    place, residual = lax.optimization_barrier(
        (jnp.stack([side, core, lax.axis_index("ulysses")]).astype(jnp.int32), residual)
    )

    send_normed, send_scaled, select = pack(
        ids_t, weights_t, norm_gain[None], residual, grad_out, experts, capacity
    )
    got_normed = exchange(send_normed)
    (got_normed, place, ids_t, weights_t, residual, grad_out, norm_gain, weight_in, weight_down) = (
        lax.optimization_barrier(
            (got_normed, place, ids_t, weights_t, residual, grad_out, norm_gain, weight_in, weight_down)
        )
    )
    got_scaled = exchange(send_scaled)
    w_in = weight_in[0]
    w_down = weight_down[0]
    keep_normed, give_normed = turn(place, got_normed, rings, span)
    came_normed = lax.ppermute(give_normed, "dp_1", SWAP)
    hidden, gate, up = forward(got_normed, w_in)
    their_hidden = lax.ppermute(hidden, "dp_1", SWAP)
    keep_scaled, give_scaled = turn(place, got_scaled, rings, span)
    came_scaled = lax.ppermute(give_scaled, "dp_1", SWAP)
    got_scaled, keep_scaled = lax.optimization_barrier((got_scaled, keep_scaled))
    mine, route = back(got_scaled, w_down, hidden, gate, up)
    theirs = lax.ppermute(mine, "dp_1", SWAP)
    keep_scaled, mine, route = lax.optimization_barrier((keep_scaled, mine, route))
    far_down, near_down = weight_rows(
        place, keep_scaled, came_scaled, hidden[None], their_hidden[None], 0, rings
    )
    came_down = lax.ppermute(far_down, "dp_0", SWAP)

    far, near = {}, {}

    def in_rows(ring, after):
        nonlocal keep_normed
        keep_normed, _ = lax.optimization_barrier((keep_normed, after))
        far[ring], near[ring] = weight_rows(place, keep_normed, came_normed, mine, theirs, ring, 1)

    in_rows(2, near_down)
    in_rows(1, near[2])
    in_rows(3, near[1])
    in_rows(0, near[3])
    (far_in, near_in), far_both, near_both = ring_sum(far, near)
    came_in = lax.ppermute(far_in.astype(jnp.bfloat16), "dp_0", SWAP)
    came_down, _, _ = lax.optimization_barrier((came_down, far_both, near_both))
    part_down = added(near_down, came_down).astype(jnp.bfloat16)
    upper = {r: part_down[r, : block // 2] for r in range(rings)}
    lower = {r: part_down[r, block // 2 :] for r in range(rings)}
    halves_down, _, _ = ring_sum(upper, lower)
    grad_down = jnp.concatenate(halves_down, axis=0)[None]

    mine, route, _ = lax.optimization_barrier((mine, route, near[3]))
    slot_normed = slot_rows(mine, w_in, experts)
    back_normed = exchange(slot_normed)
    back_route = exchange(route[:, 0].reshape(experts, capacity))
    resid = residual.astype(jnp.float32)
    inv_rms = lax.rsqrt(jnp.mean(resid * resid, axis=-1, keepdims=True) + eps)
    unit_rows = resid * inv_rms
    grad_normed = contract(select, back_normed.reshape(slot_total, width), 0, 0)
    token_route = jnp.sum(
        select.reshape(experts, capacity, tok_rows).astype(jnp.float32)
        * back_route.astype(jnp.float32)[:, :, None],
        axis=1,
    )
    chosen = ids_t[:, None, :] == lax.broadcasted_iota(jnp.int32, (1, experts, tok_rows), 1)
    route_t = jnp.sum(jnp.where(chosen, token_route[None], 0.0), axis=1)
    route_grad = (route_t / weights_t.astype(jnp.float32)).astype(jnp.bfloat16).T
    scaled_normed = grad_normed * norm_gain
    branch = inv_rms * (
        scaled_normed - unit_rows * jnp.mean(scaled_normed * unit_rows, axis=-1, keepdims=True)
    )
    grad_residual = (grad_out.astype(jnp.float32) + branch).astype(jnp.bfloat16)
    came_in, _ = lax.optimization_barrier((came_in, grad_residual))
    grad_in = near_in + came_in.astype(jnp.float32)
    return (grad_residual, route_grad, grad_in, grad_down)


def solution(mesh):
    finer = Mesh(
        mesh.devices.reshape(2, 2, mesh.shape["ulysses"], mesh.shape["expert"]),
        ("dp_0", "dp_1", "ulysses", "expert"),
    )
    return jax.shard_map(
        per_device,
        mesh=finer,
        in_specs=(
            P(DP_ULYSSES_EXPERT, None),
            P(),
            P(DP_ULYSSES_EXPERT, None),
            P(DP_ULYSSES_EXPERT, None),
            P(DP_ULYSSES_EXPERT, None),
            P("expert", None, None),
            P("expert", None, None),
        ),
        out_specs=(
            P(DP_ULYSSES_EXPERT, None),
            P(DP_ULYSSES_EXPERT, None),
            P("expert", DP_ULYSSES, None),
            P("expert", DP_ULYSSES, None),
        ),
        check_vma=False,
    )
```

```python
import jax
import jax.numpy as jnp
from jax import lax
from jax.experimental import pallas as pl
from jax.experimental.pallas import tpu as pltpu
from jax.sharding import Mesh
from jax.sharding import PartitionSpec as P


DP_ULYSSES = ("dp_0", "dp_1", "ulysses")
DP_ULYSSES_EXPERT = ("dp_0", "dp_1", "ulysses", "expert")

SWAP = [(0, 1), (1, 0)]

eps = 1e-06

VMEM = 62 * 2**20


def contract(left, right, over_left, over_right):
    return lax.dot_general(
        left, right, (((over_left,), (over_right,)), ((), ())), preferred_element_type=jnp.float32
    )


def slot_matrices(ids, weights, experts, capacity):
    tok_rows = ids.shape[1]
    expert = lax.broadcasted_iota(jnp.int32, (experts, tok_rows), 0)
    first, second = ids[0:1] == expert, ids[1:2] == expert
    hit = first | second
    weight = jnp.where(first, weights[0:1], jnp.where(second, weights[1:2], 0.0))
    square = (tok_rows, tok_rows)
    before = lax.broadcasted_iota(jnp.int32, square, 0) < lax.broadcasted_iota(jnp.int32, square, 1)
    rank = contract(
        jnp.where(hit, 1.0, 0.0).astype(jnp.bfloat16),
        jnp.where(before, 1.0, 0.0).astype(jnp.bfloat16),
        1,
        0,
    ).astype(jnp.int32)
    rank = jnp.where(hit, rank, capacity)
    slot = lax.broadcasted_iota(jnp.int32, (capacity, tok_rows), 0)
    select, scale = [], []
    for e in range(experts):
        held = rank[e : e + 1] == slot
        select.append(jnp.where(held, 1.0, 0.0))
        scale.append(jnp.where(held, weight[e : e + 1], 0.0))
    return (
        jnp.concatenate(select, axis=0).astype(jnp.bfloat16),
        jnp.concatenate(scale, axis=0).astype(jnp.bfloat16),
    )


def pack_kernel(
    ids_ref, w_ref, gain_ref, resid_ref, grad_ref, normed_ref, scaled_ref, sel_ref, inv_ref, scale_ref
):
    experts, capacity, block = normed_ref.shape

    @pl.when(pl.program_id(0) == 0)
    def _():
        full = resid_ref[...].astype(jnp.float32)
        mean = jnp.mean(full * full, axis=-1, keepdims=True)
        inv_ref[...] = lax.rsqrt(mean + eps)
        select, scale = slot_matrices(ids_ref[...], w_ref[...].astype(jnp.float32), experts, capacity)
        sel_ref[...] = select
        scale_ref[...] = scale

    at = pl.ds(pl.multiple_of(pl.program_id(0) * block, block), block)
    unit = resid_ref[:, at].astype(jnp.float32) * inv_ref[...]
    normed = (unit * gain_ref[:, at]).astype(jnp.bfloat16)
    sent = contract(sel_ref[...], normed, 1, 0).astype(jnp.bfloat16)
    normed_ref[...] = sent.reshape(experts, capacity, block)
    sent = contract(scale_ref[...], grad_ref[:, at], 1, 0).astype(jnp.bfloat16)
    scaled_ref[...] = sent.reshape(experts, capacity, block)


def pack(ids_t, w_t, gain, resid, grad, experts, capacity, block=1024):
    rows, width = resid.shape
    whole = lambda a: pl.BlockSpec(a.shape, lambda j: (0,) * a.ndim)
    args = (ids_t, w_t, gain, resid, grad)
    slots = experts * capacity
    return pl.pallas_call(
        pack_kernel,
        grid=(width // block,),
        in_specs=[whole(a) for a in args],
        out_specs=[
            pl.BlockSpec((experts, capacity, block), lambda j: (0, 0, j)),
            pl.BlockSpec((experts, capacity, block), lambda j: (0, 0, j)),
            pl.BlockSpec((slots, rows), lambda j: (0, 0)),
        ],
        out_shape=[
            jax.ShapeDtypeStruct((experts, capacity, width), jnp.bfloat16),
            jax.ShapeDtypeStruct((experts, capacity, width), jnp.bfloat16),
            jax.ShapeDtypeStruct((slots, rows), jnp.bfloat16),
        ],
        scratch_shapes=[
            pltpu.VMEM((rows, 1), jnp.float32),
            pltpu.VMEM((slots, rows), jnp.bfloat16),
        ],
        compiler_params=pltpu.CompilerParams(vmem_limit_bytes=VMEM),
        cost_estimate=pl.CostEstimate(
            flops=4 * slots * rows * width, bytes_accessed=4 * slots * width, transcendentals=0
        ),
        name="pack",
    )(*args)


def forward_kernel(got_ref, gate_w_ref, up_w_ref, hidden_ref, gate_ref, up_ref):
    parts, capacity, width = got_ref.shape
    normed = got_ref[...].reshape(parts * capacity, width)
    gate = contract(normed, gate_w_ref[...], 1, 0)
    up = contract(normed, up_w_ref[...], 1, 0)
    sigmoid = jax.nn.sigmoid(gate)
    silu = gate * sigmoid
    hidden_ref[...] = (silu * up).astype(jnp.bfloat16)
    gate_ref[...] = up * sigmoid * (1.0 + gate * (1.0 - sigmoid))
    up_ref[...] = silu


def forward(got, w_in, block=256):
    parts, capacity, width = got.shape
    slots = parts * capacity
    hidden_width = w_in.shape[1] // 2
    steps = hidden_width // block
    out = pl.BlockSpec((slots, block), lambda j: (0, j))
    return pl.pallas_call(
        forward_kernel,
        grid=(steps,),
        in_specs=[
            pl.BlockSpec(got.shape, lambda j: (0, 0, 0)),
            pl.BlockSpec((width, block), lambda j: (0, j)),
            pl.BlockSpec((width, block), lambda j: (0, steps + j)),
        ],
        out_specs=[out] * 3,
        out_shape=[
            jax.ShapeDtypeStruct((slots, hidden_width), t)
            for t in (jnp.bfloat16, jnp.float32, jnp.float32)
        ],
        compiler_params=pltpu.CompilerParams(vmem_limit_bytes=VMEM),
        cost_estimate=pl.CostEstimate(
            flops=4 * slots * hidden_width * width,
            bytes_accessed=4 * hidden_width * width + 2 * slots * width,
            transcendentals=slots * hidden_width,
        ),
        name="forward",
    )(got, w_in, w_in)


def back_kernel(got_ref, w_ref, hidden_ref, gate_ref, up_ref, out_ref, route_ref, acc_ref):
    parts, capacity, width = got_ref.shape
    grad_hidden = contract(got_ref[...].reshape(parts * capacity, width), w_ref[...], 1, 1)
    out_ref[0] = (grad_hidden * gate_ref[...]).astype(jnp.bfloat16)
    out_ref[1] = (grad_hidden * up_ref[...]).astype(jnp.bfloat16)
    part = jnp.sum(grad_hidden * hidden_ref[...].astype(jnp.float32), axis=1, keepdims=True)

    @pl.when(pl.program_id(0) == 0)
    def _():
        acc_ref[...] = part

    @pl.when(pl.program_id(0) > 0)
    def _():
        acc_ref[...] += part

    @pl.when(pl.program_id(0) == pl.num_programs(0) - 1)
    def _():
        route_ref[...] = jnp.broadcast_to(acc_ref[...], route_ref.shape).astype(jnp.bfloat16)


def back(got, w_down, hidden, gate, up, block=256):
    parts, capacity, width = got.shape
    slots = parts * capacity
    hidden_width = w_down.shape[0]
    column = pl.BlockSpec((slots, block), lambda j: (0, j))
    return pl.pallas_call(
        back_kernel,
        grid=(hidden_width // block,),
        in_specs=[
            pl.BlockSpec(got.shape, lambda j: (0, 0, 0)),
            pl.BlockSpec((block, width), lambda j: (j, 0)),
            column,
            column,
            column,
        ],
        out_specs=[
            pl.BlockSpec((2, slots, block), lambda j: (0, 0, j)),
            pl.BlockSpec((slots, 128), lambda j: (0, 0)),
        ],
        out_shape=[
            jax.ShapeDtypeStruct((2, slots, hidden_width), jnp.bfloat16),
            jax.ShapeDtypeStruct((slots, 128), jnp.bfloat16),
        ],
        scratch_shapes=[pltpu.VMEM((slots, 1), jnp.float32)],
        compiler_params=pltpu.CompilerParams(vmem_limit_bytes=VMEM),
        cost_estimate=pl.CostEstimate(
            flops=2 * slots * hidden_width * width,
            bytes_accessed=2 * hidden_width * width + 2 * slots * width + 10 * slots * hidden_width,
            transcendentals=0,
        ),
        name="back",
    )(got, w_down, hidden, gate, up)


def turn_kernel(_, keep_ref, give_ref, keep_out, give_out):
    parts, capacity, block = keep_ref.shape
    keep_out[0] = keep_ref[...].reshape(parts * capacity, block).T.reshape(keep_out.shape[1:])
    give_out[0] = give_ref[...].reshape(parts * capacity, block).T.reshape(give_out.shape[1:])


def turn(place, got, rings, span):
    parts, capacity, width = got.shape
    slots = parts * capacity
    block = width // (4 * rings)
    steps = rings // span

    def column(half, ring, place_ref, core):
        side = jnp.where(half == 0, 1 - place_ref[0], place_ref[0])
        return (0, 0, (side * 2 + core) * steps + ring)

    out = pl.BlockSpec((1, span, block, slots), lambda half, ring, _: (half, ring, 0, 0))
    return pl.pallas_call(
        turn_kernel,
        grid_spec=pltpu.PrefetchScalarGridSpec(
            num_scalar_prefetch=1,
            grid=(2, steps),
            in_specs=[
                pl.BlockSpec(
                    (parts, capacity, span * block),
                    lambda half, ring, at: column(half, ring, at, at[1]),
                ),
                pl.BlockSpec(
                    (parts, capacity, span * block),
                    lambda half, ring, at: column(half, ring, at, 1 - at[1]),
                ),
            ],
            out_specs=[out, out],
        ),
        out_shape=[jax.ShapeDtypeStruct((2, rings, block, slots), jnp.bfloat16)] * 2,
        compiler_params=pltpu.CompilerParams(vmem_limit_bytes=VMEM),
        cost_estimate=pl.CostEstimate(
            flops=slots * width * 1024, bytes_accessed=4 * slots * width, transcendentals=0
        ),
        name="turn",
    )(place, got, got)


def rows_kernel(_, keep_ref, came_ref, mine_ref, theirs_ref, far_ref, near_ref):
    block, slots = keep_ref.shape[2:]
    keep, came = keep_ref[...].reshape(2 * block, slots), came_ref[...].reshape(2 * block, slots)
    rows = contract(keep, mine_ref[0], 1, 0) + contract(came, theirs_ref[0], 1, 0)
    rows = rows.astype(jnp.bfloat16)
    far_ref[0] = rows[:block]
    near_ref[0] = rows[block:]


def weight_rows(place, keep, came, mine, theirs, first, count):
    _, rings, block, slots = keep.shape
    units, _, width = mine.shape
    left = pl.BlockSpec(
        (2, 1, block, slots), lambda i, u, at: (0, lax.rem(at[2] + (first + i), rings), 0, 0)
    )
    right = pl.BlockSpec((1, slots, width), lambda i, u, at: (u, 0, 0))
    out = pl.BlockSpec((1, block, width), lambda i, u, at: (i, 0, u))
    return pl.pallas_call(
        rows_kernel,
        grid_spec=pltpu.PrefetchScalarGridSpec(
            num_scalar_prefetch=1,
            grid=(count, units),
            in_specs=[left, left, right, right],
            out_specs=[out, out],
        ),
        out_shape=[jax.ShapeDtypeStruct((count, block, units * width), jnp.bfloat16)] * 2,
        compiler_params=pltpu.CompilerParams(vmem_limit_bytes=VMEM),
        cost_estimate=pl.CostEstimate(
            flops=8 * count * block * mine.size,
            bytes_accessed=4 * mine.size + 4 * count * block * (2 * slots + units * width),
            transcendentals=0,
        ),
    )(place, keep, came, mine, theirs)


SEND_ORDER = (2, 1, 3, 0)


def ring_at(step):
    ring = SEND_ORDER[-1]
    for at, value in enumerate(SEND_ORDER[:-1]):
        ring = jnp.where(step == at, value, ring)
    return ring


def messages_kernel(_, keep_ref, came_ref, mine_ref, theirs_ref, *out_refs):
    block, slots = keep_ref.shape[2:]
    unit = pl.program_id(1)
    keep, came = keep_ref[...].reshape(2 * block, slots), came_ref[...].reshape(2 * block, slots)
    rows = contract(keep, mine_ref[unit], 1, 0) + contract(came, theirs_ref[unit], 1, 0)
    rows = rows.astype(jnp.bfloat16)
    for at in range(len(SEND_ORDER)):

        @pl.when(pl.program_id(0) == at)
        def _():
            out_refs[2 * at][0] = rows[:block]
            out_refs[2 * at + 1][0] = rows[block:]


def weight_messages(place, keep, came, mine, theirs):
    _, rings, block, slots = keep.shape
    units, _, width = mine.shape
    left = pl.BlockSpec(
        (2, 1, block, slots), lambda i, u, at: (0, lax.rem(at[2] + ring_at(i), rings), 0, 0)
    )
    right = pl.BlockSpec(mine.shape, lambda i, u, at: (0, 0, 0))

    def out(k):
        return pl.BlockSpec(
            (1, block, width),
            lambda i, u, at: (0, 0, jnp.where(i == k, u, jnp.where(i < k, 0, units - 1))),
        )

    outs = pl.pallas_call(
        messages_kernel,
        grid_spec=pltpu.PrefetchScalarGridSpec(
            num_scalar_prefetch=1,
            grid=(rings, units),
            in_specs=[left, left, right, right],
            out_specs=[out(k) for k in range(rings) for _ in range(2)],
        ),
        out_shape=[jax.ShapeDtypeStruct((1, block, units * width), jnp.bfloat16)] * (2 * rings),
        compiler_params=pltpu.CompilerParams(vmem_limit_bytes=VMEM),
        cost_estimate=pl.CostEstimate(
            flops=8 * rings * block * mine.size,
            bytes_accessed=4 * mine.size + 4 * rings * block * (2 * slots + units * width),
            transcendentals=0,
        ),
        name="grad_in",
    )(place, keep, came, mine, theirs)
    far = {ring: outs[2 * k] for k, ring in enumerate(SEND_ORDER)}
    near = {ring: outs[2 * k + 1] for k, ring in enumerate(SEND_ORDER)}
    return far, near


def slot_kernel(grads_ref, w_ref, out_ref):
    width = grads_ref.shape[2]
    rows = contract(grads_ref[0], w_ref[:, :width], 1, 1) + contract(
        grads_ref[1], w_ref[:, width:], 1, 1
    )
    out_ref[...] = rows.astype(jnp.bfloat16).reshape(out_ref.shape)


def slot_rows(grads, w_in, parts, block=1024):
    _, slots, hidden_width = grads.shape
    width = w_in.shape[0]
    return pl.pallas_call(
        slot_kernel,
        grid=(width // block,),
        in_specs=[
            pl.BlockSpec(grads.shape, lambda j: (0, 0, 0)),
            pl.BlockSpec((block, 2 * hidden_width), lambda j: (j, 0)),
        ],
        out_specs=pl.BlockSpec((parts, slots // parts, block), lambda j: (0, 0, j)),
        out_shape=jax.ShapeDtypeStruct((parts, slots // parts, width), jnp.bfloat16),
        compiler_params=pltpu.CompilerParams(vmem_limit_bytes=VMEM),
        cost_estimate=pl.CostEstimate(
            flops=4 * slots * hidden_width * width,
            bytes_accessed=4 * hidden_width * width + 2 * slots * width,
            transcendentals=0,
        ),
        name="slot_rows",
    )(grads, w_in)


def added(*terms):
    return sum(t.astype(jnp.float32) for t in terms)


def ring_sum(low, high):
    size = lax.axis_size("ulysses")
    ahead = [(i, (i + 1) % size) for i in range(size)]
    behind = [(i, (i - 1) % size) for i in range(size)]
    low_two = lax.ppermute(low[2], "ulysses", ahead)
    high_two = lax.ppermute(high[2], "ulysses", behind)
    high_side = lax.ppermute(high[1], "ulysses", ahead)
    low_side = lax.ppermute(low[3], "ulysses", behind)
    low_both = added(low[1], low_two).astype(jnp.bfloat16)
    high_both = added(high[3], high_two).astype(jnp.bfloat16)
    low_last = lax.ppermute(low_both, "ulysses", ahead)
    high_last = lax.ppermute(high_both, "ulysses", behind)
    sums = added(low[0], low_last, low_side), added(high[0], high_last, high_side)
    return sums, low_both, high_both


def exchange(rows):
    experts = lax.axis_size("expert")
    groups = [[(g ^ (e & 1)) * experts + e for e in range(experts)] for g in range(2)]
    return lax.all_to_all(
        rows,
        ("dp_0", "expert"),
        split_axis=0,
        concat_axis=0,
        axis_index_groups=groups,
        tiled=True,
    )


def per_device(residual, norm_gain, grad_out, expert_ids, route_weights, weight_in, weight_down):
    tok_rows, width = residual.shape
    topk = expert_ids.shape[1]
    experts = lax.axis_size("expert")
    capacity = min(tok_rows, 3 * tok_rows * topk // (2 * experts))
    slot_total = experts * capacity
    rings = lax.axis_size("ulysses")
    block = width // (4 * rings)
    span = 2 if rings % 2 == 0 else 1
    side = lax.axis_index("dp_0")
    core = lax.axis_index("dp_1")
    ids_t = expert_ids.T
    weights_t = route_weights.T
    place, residual = lax.optimization_barrier(
        (jnp.stack([side, core, lax.axis_index("ulysses")]).astype(jnp.int32), residual)
    )

    send_normed, send_scaled, select = pack(
        ids_t, weights_t, norm_gain[None], residual, grad_out, experts, capacity
    )
    got_normed = exchange(send_normed)
    (got_normed, place, ids_t, weights_t, residual, grad_out, norm_gain, weight_in, weight_down) = (
        lax.optimization_barrier(
            (got_normed, place, ids_t, weights_t, residual, grad_out, norm_gain, weight_in, weight_down)
        )
    )
    got_scaled = exchange(send_scaled)
    w_in = weight_in[0]
    w_down = weight_down[0]
    keep_normed, give_normed = turn(place, got_normed, rings, span)
    came_normed = lax.ppermute(give_normed, "dp_1", SWAP)
    hidden, gate, up = forward(got_normed, w_in)
    their_hidden = lax.ppermute(hidden, "dp_1", SWAP)
    mine, route = back(got_scaled, w_down, hidden, gate, up)
    theirs = lax.ppermute(mine, "dp_1", SWAP)
    got_scaled, mine, route = lax.optimization_barrier((got_scaled, mine, route))
    keep_scaled, give_scaled = turn(place, got_scaled, rings, span)
    came_scaled = lax.ppermute(give_scaled, "dp_1", SWAP)
    keep_normed, keep_scaled = lax.optimization_barrier((keep_normed, keep_scaled))
    far, near = weight_messages(place, keep_normed, came_normed, mine, theirs)
    keep_scaled, _ = lax.optimization_barrier((keep_scaled, near[0]))
    far_down, near_down = weight_rows(
        place, keep_scaled, came_scaled, hidden[None], their_hidden[None], 0, rings
    )
    came_down = lax.ppermute(far_down, "dp_0", SWAP)
    (far_in, near_in), far_both, near_both = ring_sum(far, near)
    came_in = lax.ppermute(far_in.astype(jnp.bfloat16), "dp_0", SWAP)
    came_down, _, _ = lax.optimization_barrier((came_down, far_both, near_both))
    part_down = added(near_down, came_down).astype(jnp.bfloat16)
    upper = {r: part_down[r, : block // 2] for r in range(rings)}
    lower = {r: part_down[r, block // 2 :] for r in range(rings)}
    halves_down, _, _ = ring_sum(upper, lower)
    grad_down = jnp.concatenate(halves_down, axis=0)[None]

    mine, route, _ = lax.optimization_barrier((mine, route, near_down))
    slot_normed = slot_rows(mine, w_in, experts)
    back_normed = exchange(slot_normed)
    back_route = exchange(route[:, 0].reshape(experts, capacity))
    resid = residual.astype(jnp.float32)
    inv_rms = lax.rsqrt(jnp.mean(resid * resid, axis=-1, keepdims=True) + eps)
    unit_rows = resid * inv_rms
    grad_normed = contract(select, back_normed.reshape(slot_total, width), 0, 0)
    token_route = jnp.sum(
        select.reshape(experts, capacity, tok_rows).astype(jnp.float32)
        * back_route.astype(jnp.float32)[:, :, None],
        axis=1,
    )
    chosen = ids_t[:, None, :] == lax.broadcasted_iota(jnp.int32, (1, experts, tok_rows), 1)
    route_t = jnp.sum(jnp.where(chosen, token_route[None], 0.0), axis=1)
    route_grad = (route_t / weights_t.astype(jnp.float32)).astype(jnp.bfloat16).T
    scaled_normed = grad_normed * norm_gain
    branch = inv_rms * (
        scaled_normed - unit_rows * jnp.mean(scaled_normed * unit_rows, axis=-1, keepdims=True)
    )
    grad_residual = (grad_out.astype(jnp.float32) + branch).astype(jnp.bfloat16)
    came_in, _ = lax.optimization_barrier((came_in, grad_residual))
    grad_in = near_in + came_in.astype(jnp.float32)
    return (grad_residual, route_grad, grad_in, grad_down)


def solution(mesh):
    finer = Mesh(
        mesh.devices.reshape(2, 2, mesh.shape["ulysses"], mesh.shape["expert"]),
        ("dp_0", "dp_1", "ulysses", "expert"),
    )
    return jax.shard_map(
        per_device,
        mesh=finer,
        in_specs=(
            P(DP_ULYSSES_EXPERT, None),
            P(),
            P(DP_ULYSSES_EXPERT, None),
            P(DP_ULYSSES_EXPERT, None),
            P(DP_ULYSSES_EXPERT, None),
            P("expert", None, None),
            P("expert", None, None),
        ),
        out_specs=(
            P(DP_ULYSSES_EXPERT, None),
            P(DP_ULYSSES_EXPERT, None),
            P("expert", DP_ULYSSES, None),
            P("expert", DP_ULYSSES, None),
        ),
        check_vma=False,
    )
```

```python
import jax
import jax.numpy as jnp
from jax import lax
from jax.experimental import pallas as pl
from jax.experimental.pallas import tpu as pltpu
from jax.sharding import Mesh
from jax.sharding import PartitionSpec as P


DP_ULYSSES = ("dp_0", "dp_1", "ulysses")
DP_ULYSSES_EXPERT = ("dp_0", "dp_1", "ulysses", "expert")

SWAP = [(0, 1), (1, 0)]

eps = 1e-06

VMEM = 62 * 2**20


def contract(left, right, over_left, over_right):
    return lax.dot_general(
        left, right, (((over_left,), (over_right,)), ((), ())), preferred_element_type=jnp.float32
    )


def slot_matrices(ids, weights, experts, capacity):
    tok_rows = ids.shape[1]
    expert = lax.broadcasted_iota(jnp.int32, (experts, tok_rows), 0)
    first, second = ids[0:1] == expert, ids[1:2] == expert
    hit = first | second
    weight = jnp.where(first, weights[0:1], jnp.where(second, weights[1:2], 0.0))
    square = (tok_rows, tok_rows)
    before = lax.broadcasted_iota(jnp.int32, square, 0) < lax.broadcasted_iota(jnp.int32, square, 1)
    rank = contract(
        jnp.where(hit, 1.0, 0.0).astype(jnp.bfloat16),
        jnp.where(before, 1.0, 0.0).astype(jnp.bfloat16),
        1,
        0,
    ).astype(jnp.int32)
    rank = jnp.where(hit, rank, capacity)
    slot = lax.broadcasted_iota(jnp.int32, (capacity, tok_rows), 0)
    select, scale = [], []
    for e in range(experts):
        held = rank[e : e + 1] == slot
        select.append(jnp.where(held, 1.0, 0.0))
        scale.append(jnp.where(held, weight[e : e + 1], 0.0))
    return (
        jnp.concatenate(select, axis=0).astype(jnp.bfloat16),
        jnp.concatenate(scale, axis=0).astype(jnp.bfloat16),
    )


def shifted(expert, step, sign):
    return (expert // 2 + sign * (step // 2) + 4) % 4 * 2 + (expert + step) % 2


def pack_kernel(place_ref, ids_ref, w_ref, gain_ref, resid_ref, grad_ref, *out_refs):
    *normed_refs, scaled_ref, sel_ref, inv_ref, scale_ref, turned_ref = out_refs
    experts, capacity, block = scaled_ref.shape

    @pl.when(pl.program_id(0) == 0)
    def _():
        full = resid_ref[...].astype(jnp.float32)
        mean = jnp.mean(full * full, axis=-1, keepdims=True)
        inv_ref[...] = lax.rsqrt(mean + eps)
        select, scale = slot_matrices(ids_ref[...], w_ref[...].astype(jnp.float32), experts, capacity)
        sel_ref[...] = select
        scale_ref[...] = scale
        for step in range(experts):
            start = pl.multiple_of(shifted(place_ref[3], step, 1) * capacity, 16)
            turned_ref[step * capacity : (step + 1) * capacity] = sel_ref[pl.ds(start, capacity)]

    at = pl.ds(pl.multiple_of(pl.program_id(0) * block, block), block)
    unit = resid_ref[:, at].astype(jnp.float32) * inv_ref[...]
    normed = (unit * gain_ref[:, at]).astype(jnp.bfloat16)
    sent = contract(turned_ref[...], normed, 1, 0).astype(jnp.bfloat16)
    for step in range(experts):
        normed_refs[step][...] = sent[step * capacity : (step + 1) * capacity]
    sent = contract(scale_ref[...], grad_ref[:, at], 1, 0).astype(jnp.bfloat16)
    scaled_ref[...] = sent.reshape(experts, capacity, block)


def pack(place, ids_t, w_t, gain, resid, grad, experts, capacity, block=1024):
    rows, width = resid.shape
    args = (ids_t, w_t, gain, resid, grad)
    slots = experts * capacity
    return pl.pallas_call(
        pack_kernel,
        grid_spec=pltpu.PrefetchScalarGridSpec(
            num_scalar_prefetch=1,
            grid=(width // block,),
            in_specs=[pl.BlockSpec(a.shape, lambda j, _: (0, 0)) for a in args],
            out_specs=[pl.BlockSpec((capacity, block), lambda j, _: (0, j))] * experts
            + [
                pl.BlockSpec((experts, capacity, block), lambda j, _: (0, 0, j)),
                pl.BlockSpec((slots, rows), lambda j, _: (0, 0)),
            ],
            scratch_shapes=[
                pltpu.VMEM((rows, 1), jnp.float32),
                pltpu.VMEM((slots, rows), jnp.bfloat16),
                pltpu.VMEM((slots, rows), jnp.bfloat16),
            ],
        ),
        out_shape=[jax.ShapeDtypeStruct((capacity, width), jnp.bfloat16)] * experts
        + [
            jax.ShapeDtypeStruct((experts, capacity, width), jnp.bfloat16),
            jax.ShapeDtypeStruct((slots, rows), jnp.bfloat16),
        ],
        compiler_params=pltpu.CompilerParams(vmem_limit_bytes=VMEM),
        cost_estimate=pl.CostEstimate(
            flops=4 * slots * rows * width, bytes_accessed=4 * slots * width, transcendentals=0
        ),
        name="pack",
    )(place, *args)


def gather_kernel(place_ref, *refs):
    *block_refs, out_ref = refs
    for step, block_ref in enumerate(block_refs):
        out_ref[shifted(place_ref[3], step, -1)] = block_ref[...]


def gather(place, blocks, block=1024):
    capacity, width = blocks[0].shape
    experts = len(blocks)
    return pl.pallas_call(
        gather_kernel,
        grid_spec=pltpu.PrefetchScalarGridSpec(
            num_scalar_prefetch=1,
            grid=(width // block,),
            in_specs=[pl.BlockSpec((capacity, block), lambda j, _: (0, j))] * experts,
            out_specs=pl.BlockSpec((experts, capacity, block), lambda j, _: (0, 0, j)),
        ),
        out_shape=jax.ShapeDtypeStruct((experts, capacity, width), jnp.bfloat16),
        compiler_params=pltpu.CompilerParams(vmem_limit_bytes=VMEM),
        cost_estimate=pl.CostEstimate(
            flops=experts * capacity * width * 256,
            bytes_accessed=4 * experts * capacity * width,
            transcendentals=0,
        ),
        name="gather",
    )(place, *blocks)


def forward_kernel(got_ref, gate_w_ref, up_w_ref, hidden_ref, gate_ref, up_ref):
    parts, capacity, width = got_ref.shape
    normed = got_ref[...].reshape(parts * capacity, width)
    gate = contract(normed, gate_w_ref[...], 1, 0)
    up = contract(normed, up_w_ref[...], 1, 0)
    sigmoid = jax.nn.sigmoid(gate)
    silu = gate * sigmoid
    hidden_ref[...] = (silu * up).astype(jnp.bfloat16)
    gate_ref[...] = up * sigmoid * (1.0 + gate * (1.0 - sigmoid))
    up_ref[...] = silu


def forward(got, w_in, block=256):
    parts, capacity, width = got.shape
    slots = parts * capacity
    hidden_width = w_in.shape[1] // 2
    steps = hidden_width // block
    out = pl.BlockSpec((slots, block), lambda j: (0, j))
    return pl.pallas_call(
        forward_kernel,
        grid=(steps,),
        in_specs=[
            pl.BlockSpec(got.shape, lambda j: (0, 0, 0)),
            pl.BlockSpec((width, block), lambda j: (0, j)),
            pl.BlockSpec((width, block), lambda j: (0, steps + j)),
        ],
        out_specs=[out] * 3,
        out_shape=[
            jax.ShapeDtypeStruct((slots, hidden_width), t)
            for t in (jnp.bfloat16, jnp.float32, jnp.float32)
        ],
        compiler_params=pltpu.CompilerParams(vmem_limit_bytes=VMEM),
        cost_estimate=pl.CostEstimate(
            flops=4 * slots * hidden_width * width,
            bytes_accessed=4 * hidden_width * width + 2 * slots * width,
            transcendentals=slots * hidden_width,
        ),
        name="forward",
    )(got, w_in, w_in)


def back_kernel(got_ref, w_ref, hidden_ref, gate_ref, up_ref, out_ref, route_ref, acc_ref):
    parts, capacity, width = got_ref.shape
    grad_hidden = contract(got_ref[...].reshape(parts * capacity, width), w_ref[...], 1, 1)
    out_ref[0] = (grad_hidden * gate_ref[...]).astype(jnp.bfloat16)
    out_ref[1] = (grad_hidden * up_ref[...]).astype(jnp.bfloat16)
    part = jnp.sum(grad_hidden * hidden_ref[...].astype(jnp.float32), axis=1, keepdims=True)

    @pl.when(pl.program_id(0) == 0)
    def _():
        acc_ref[...] = part

    @pl.when(pl.program_id(0) > 0)
    def _():
        acc_ref[...] += part

    @pl.when(pl.program_id(0) == pl.num_programs(0) - 1)
    def _():
        route_ref[...] = jnp.broadcast_to(acc_ref[...], route_ref.shape).astype(jnp.bfloat16)


def back(got, w_down, hidden, gate, up, block=256):
    parts, capacity, width = got.shape
    slots = parts * capacity
    hidden_width = w_down.shape[0]
    column = pl.BlockSpec((slots, block), lambda j: (0, j))
    return pl.pallas_call(
        back_kernel,
        grid=(hidden_width // block,),
        in_specs=[
            pl.BlockSpec(got.shape, lambda j: (0, 0, 0)),
            pl.BlockSpec((block, width), lambda j: (j, 0)),
            column,
            column,
            column,
        ],
        out_specs=[
            pl.BlockSpec((2, slots, block), lambda j: (0, 0, j)),
            pl.BlockSpec((slots, 128), lambda j: (0, 0)),
        ],
        out_shape=[
            jax.ShapeDtypeStruct((2, slots, hidden_width), jnp.bfloat16),
            jax.ShapeDtypeStruct((slots, 128), jnp.bfloat16),
        ],
        scratch_shapes=[pltpu.VMEM((slots, 1), jnp.float32)],
        compiler_params=pltpu.CompilerParams(vmem_limit_bytes=VMEM),
        cost_estimate=pl.CostEstimate(
            flops=2 * slots * hidden_width * width,
            bytes_accessed=2 * hidden_width * width + 2 * slots * width + 10 * slots * hidden_width,
            transcendentals=0,
        ),
        name="back",
    )(got, w_down, hidden, gate, up)


def turn_kernel(_, keep_ref, give_ref, keep_out, give_out):
    parts, capacity, block = keep_ref.shape
    keep_out[0] = keep_ref[...].reshape(parts * capacity, block).T.reshape(keep_out.shape[1:])
    give_out[0] = give_ref[...].reshape(parts * capacity, block).T.reshape(give_out.shape[1:])


def turn(place, got, rings, span):
    parts, capacity, width = got.shape
    slots = parts * capacity
    block = width // (4 * rings)
    steps = rings // span

    def column(half, ring, place_ref, core):
        side = jnp.where(half == 0, 1 - place_ref[0], place_ref[0])
        return (0, 0, (side * 2 + core) * steps + ring)

    out = pl.BlockSpec((1, span, block, slots), lambda half, ring, _: (half, ring, 0, 0))
    return pl.pallas_call(
        turn_kernel,
        grid_spec=pltpu.PrefetchScalarGridSpec(
            num_scalar_prefetch=1,
            grid=(2, steps),
            in_specs=[
                pl.BlockSpec(
                    (parts, capacity, span * block),
                    lambda half, ring, at: column(half, ring, at, at[1]),
                ),
                pl.BlockSpec(
                    (parts, capacity, span * block),
                    lambda half, ring, at: column(half, ring, at, 1 - at[1]),
                ),
            ],
            out_specs=[out, out],
        ),
        out_shape=[jax.ShapeDtypeStruct((2, rings, block, slots), jnp.bfloat16)] * 2,
        compiler_params=pltpu.CompilerParams(vmem_limit_bytes=VMEM),
        cost_estimate=pl.CostEstimate(
            flops=slots * width * 1024, bytes_accessed=4 * slots * width, transcendentals=0
        ),
        name="turn",
    )(place, got, got)


def rows_kernel(_, keep_ref, came_ref, mine_ref, theirs_ref, far_ref, near_ref):
    block, slots = keep_ref.shape[2:]
    keep, came = keep_ref[...].reshape(2 * block, slots), came_ref[...].reshape(2 * block, slots)
    rows = contract(keep, mine_ref[0], 1, 0) + contract(came, theirs_ref[0], 1, 0)
    rows = rows.astype(jnp.bfloat16)
    far_ref[0] = rows[:block]
    near_ref[0] = rows[block:]


def weight_rows(place, keep, came, mine, theirs, first, count):
    _, rings, block, slots = keep.shape
    units, _, width = mine.shape
    left = pl.BlockSpec(
        (2, 1, block, slots), lambda i, u, at: (0, lax.rem(at[2] + (first + i), rings), 0, 0)
    )
    right = pl.BlockSpec((1, slots, width), lambda i, u, at: (u, 0, 0))
    out = pl.BlockSpec((1, block, width), lambda i, u, at: (i, 0, u))
    return pl.pallas_call(
        rows_kernel,
        grid_spec=pltpu.PrefetchScalarGridSpec(
            num_scalar_prefetch=1,
            grid=(count, units),
            in_specs=[left, left, right, right],
            out_specs=[out, out],
        ),
        out_shape=[jax.ShapeDtypeStruct((count, block, units * width), jnp.bfloat16)] * 2,
        compiler_params=pltpu.CompilerParams(vmem_limit_bytes=VMEM),
        cost_estimate=pl.CostEstimate(
            flops=8 * count * block * mine.size,
            bytes_accessed=4 * mine.size + 4 * count * block * (2 * slots + units * width),
            transcendentals=0,
        ),
    )(place, keep, came, mine, theirs)


SEND_ORDER = (2, 1, 3, 0)


def ring_at(step):
    ring = SEND_ORDER[-1]
    for at, value in enumerate(SEND_ORDER[:-1]):
        ring = jnp.where(step == at, value, ring)
    return ring


def messages_kernel(_, keep_ref, came_ref, mine_ref, theirs_ref, *out_refs):
    block, slots = keep_ref.shape[2:]
    units, _, width = mine_ref.shape
    keep, came = keep_ref[...].reshape(2 * block, slots), came_ref[...].reshape(2 * block, slots)
    for unit in range(units):
        columns = slice(unit * width, (unit + 1) * width)
        rows = contract(keep, mine_ref[unit], 1, 0) + contract(came, theirs_ref[unit], 1, 0)
        rows = rows.astype(jnp.bfloat16)
        for at in range(len(SEND_ORDER)):

            @pl.when(pl.program_id(0) == at)
            def _():
                out_refs[2 * at][0, :, columns] = rows[:block]
                out_refs[2 * at + 1][0, :, columns] = rows[block:]


def weight_messages(place, keep, came, mine, theirs):
    _, rings, block, slots = keep.shape
    units, _, width = mine.shape
    left = pl.BlockSpec(
        (2, 1, block, slots), lambda i, at: (0, lax.rem(at[2] + ring_at(i), rings), 0, 0)
    )
    right = pl.BlockSpec(mine.shape, lambda i, at: (0, 0, 0))
    outs = pl.pallas_call(
        messages_kernel,
        grid_spec=pltpu.PrefetchScalarGridSpec(
            num_scalar_prefetch=1,
            grid=(rings,),
            in_specs=[left, left, right, right],
            out_specs=[pl.BlockSpec((1, block, units * width), lambda i, at: (0, 0, 0))]
            * (2 * rings),
        ),
        out_shape=[jax.ShapeDtypeStruct((1, block, units * width), jnp.bfloat16)] * (2 * rings),
        compiler_params=pltpu.CompilerParams(vmem_limit_bytes=VMEM),
        cost_estimate=pl.CostEstimate(
            flops=8 * rings * block * mine.size,
            bytes_accessed=4 * mine.size + 4 * rings * block * (2 * slots + units * width),
            transcendentals=0,
        ),
        name="grad_in",
    )(place, keep, came, mine, theirs)
    far = {ring: outs[2 * k] for k, ring in enumerate(SEND_ORDER)}
    near = {ring: outs[2 * k + 1] for k, ring in enumerate(SEND_ORDER)}
    return far, near


def slot_kernel(grads_ref, w_ref, out_ref):
    width = grads_ref.shape[2]
    rows = contract(grads_ref[0], w_ref[:, :width], 1, 1) + contract(
        grads_ref[1], w_ref[:, width:], 1, 1
    )
    out_ref[...] = rows.astype(jnp.bfloat16).reshape(out_ref.shape)


def slot_rows(grads, w_in, parts, block=1024):
    _, slots, hidden_width = grads.shape
    width = w_in.shape[0]
    return pl.pallas_call(
        slot_kernel,
        grid=(width // block,),
        in_specs=[
            pl.BlockSpec(grads.shape, lambda j: (0, 0, 0)),
            pl.BlockSpec((block, 2 * hidden_width), lambda j: (j, 0)),
        ],
        out_specs=pl.BlockSpec((parts, slots // parts, block), lambda j: (0, 0, j)),
        out_shape=jax.ShapeDtypeStruct((parts, slots // parts, width), jnp.bfloat16),
        compiler_params=pltpu.CompilerParams(vmem_limit_bytes=VMEM),
        cost_estimate=pl.CostEstimate(
            flops=4 * slots * hidden_width * width,
            bytes_accessed=4 * hidden_width * width + 2 * slots * width,
            transcendentals=0,
        ),
        name="slot_rows",
    )(grads, w_in)


def displaced(rows, step):
    experts = lax.axis_size("expert")
    pairs = [
        (side * experts + e, (side + step) % 2 * experts + shifted(e, step, 1))
        for side in range(2)
        for e in range(experts)
    ]
    return lax.ppermute(rows, ("dp_0", "expert"), pairs)


def added(*terms):
    return sum(t.astype(jnp.float32) for t in terms)


def ring_sum(low, high):
    size = lax.axis_size("ulysses")
    ahead = [(i, (i + 1) % size) for i in range(size)]
    behind = [(i, (i - 1) % size) for i in range(size)]
    low_two = lax.ppermute(low[2], "ulysses", ahead)
    high_two = lax.ppermute(high[2], "ulysses", behind)
    high_side = lax.ppermute(high[1], "ulysses", ahead)
    low_side = lax.ppermute(low[3], "ulysses", behind)
    low_both = added(low[1], low_two).astype(jnp.bfloat16)
    high_both = added(high[3], high_two).astype(jnp.bfloat16)
    low_last = lax.ppermute(low_both, "ulysses", ahead)
    high_last = lax.ppermute(high_both, "ulysses", behind)
    sums = added(low[0], low_last, low_side), added(high[0], high_last, high_side)
    return sums, low_both, high_both


def exchange(rows):
    experts = lax.axis_size("expert")
    groups = [[(g ^ (e & 1)) * experts + e for e in range(experts)] for g in range(2)]
    return lax.all_to_all(
        rows,
        ("dp_0", "expert"),
        split_axis=0,
        concat_axis=0,
        axis_index_groups=groups,
        tiled=True,
    )


def per_device(residual, norm_gain, grad_out, expert_ids, route_weights, weight_in, weight_down):
    tok_rows, width = residual.shape
    topk = expert_ids.shape[1]
    experts = lax.axis_size("expert")
    capacity = min(tok_rows, 3 * tok_rows * topk // (2 * experts))
    slot_total = experts * capacity
    rings = lax.axis_size("ulysses")
    block = width // (4 * rings)
    span = 2 if rings % 2 == 0 else 1
    side = lax.axis_index("dp_0")
    core = lax.axis_index("dp_1")
    ids_t = expert_ids.T
    weights_t = route_weights.T
    place, residual = lax.optimization_barrier(
        (
            jnp.stack([side, core, lax.axis_index("ulysses"), lax.axis_index("expert")]).astype(
                jnp.int32
            ),
            residual,
        )
    )

    *send_normed, send_scaled, select = pack(
        place, ids_t, weights_t, norm_gain[None], residual, grad_out, experts, capacity
    )
    blocks = send_normed[:1] + [displaced(send_normed[k], k) for k in range(1, experts)]
    got_scaled = exchange(send_scaled)
    got_normed = gather(place, blocks)
    w_in = weight_in[0]
    w_down = weight_down[0]
    keep_normed, give_normed = turn(place, got_normed, rings, span)
    came_normed = lax.ppermute(give_normed, "dp_1", SWAP)
    hidden, gate, up = forward(got_normed, w_in)
    their_hidden = lax.ppermute(hidden, "dp_1", SWAP)
    mine, route = back(got_scaled, w_down, hidden, gate, up)
    theirs = lax.ppermute(mine, "dp_1", SWAP)
    got_scaled, mine, route = lax.optimization_barrier((got_scaled, mine, route))
    keep_scaled, give_scaled = turn(place, got_scaled, rings, span)
    came_scaled = lax.ppermute(give_scaled, "dp_1", SWAP)
    keep_normed, keep_scaled = lax.optimization_barrier((keep_normed, keep_scaled))
    far, near = weight_messages(place, keep_normed, came_normed, mine, theirs)
    keep_scaled, _ = lax.optimization_barrier((keep_scaled, near[0]))
    far_down, near_down = weight_rows(
        place, keep_scaled, came_scaled, hidden[None], their_hidden[None], 0, rings
    )
    came_down = lax.ppermute(far_down, "dp_0", SWAP)
    (far_in, near_in), far_both, near_both = ring_sum(far, near)
    came_in = lax.ppermute(far_in.astype(jnp.bfloat16), "dp_0", SWAP)
    came_down, _, _ = lax.optimization_barrier((came_down, far_both, near_both))
    part_down = added(near_down, came_down).astype(jnp.bfloat16)
    upper = {r: part_down[r, : block // 2] for r in range(rings)}
    lower = {r: part_down[r, block // 2 :] for r in range(rings)}
    halves_down, _, _ = ring_sum(upper, lower)
    grad_down = jnp.concatenate(halves_down, axis=0)[None]

    mine, route, _ = lax.optimization_barrier((mine, route, near_down))
    slot_normed = slot_rows(mine, w_in, experts)
    back_normed = exchange(slot_normed)
    back_route = exchange(route[:, 0].reshape(experts, capacity))
    resid = residual.astype(jnp.float32)
    inv_rms = lax.rsqrt(jnp.mean(resid * resid, axis=-1, keepdims=True) + eps)
    unit_rows = resid * inv_rms
    grad_normed = contract(select, back_normed.reshape(slot_total, width), 0, 0)
    token_route = jnp.sum(
        select.reshape(experts, capacity, tok_rows).astype(jnp.float32)
        * back_route.astype(jnp.float32)[:, :, None],
        axis=1,
    )
    chosen = ids_t[:, None, :] == lax.broadcasted_iota(jnp.int32, (1, experts, tok_rows), 1)
    route_t = jnp.sum(jnp.where(chosen, token_route[None], 0.0), axis=1)
    route_grad = (route_t / weights_t.astype(jnp.float32)).astype(jnp.bfloat16).T
    scaled_normed = grad_normed * norm_gain
    branch = inv_rms * (
        scaled_normed - unit_rows * jnp.mean(scaled_normed * unit_rows, axis=-1, keepdims=True)
    )
    grad_residual = (grad_out.astype(jnp.float32) + branch).astype(jnp.bfloat16)
    came_in, _ = lax.optimization_barrier((came_in, grad_residual))
    grad_in = near_in + came_in.astype(jnp.float32)
    return (grad_residual, route_grad, grad_in, grad_down)


def solution(mesh):
    finer = Mesh(
        mesh.devices.reshape(2, 2, mesh.shape["ulysses"], mesh.shape["expert"]),
        ("dp_0", "dp_1", "ulysses", "expert"),
    )
    return jax.shard_map(
        per_device,
        mesh=finer,
        in_specs=(
            P(DP_ULYSSES_EXPERT, None),
            P(),
            P(DP_ULYSSES_EXPERT, None),
            P(DP_ULYSSES_EXPERT, None),
            P(DP_ULYSSES_EXPERT, None),
            P("expert", None, None),
            P("expert", None, None),
        ),
        out_specs=(
            P(DP_ULYSSES_EXPERT, None),
            P(DP_ULYSSES_EXPERT, None),
            P("expert", DP_ULYSSES, None),
            P("expert", DP_ULYSSES, None),
        ),
        check_vma=False,
    )
```

```python
import jax
import jax.numpy as jnp
from jax import lax
from jax.experimental import pallas as pl
from jax.experimental.pallas import tpu as pltpu
from jax.sharding import Mesh
from jax.sharding import PartitionSpec as P


DP_ULYSSES = ("dp_0", "dp_1", "ulysses")
DP_ULYSSES_EXPERT = ("dp_0", "dp_1", "ulysses", "expert")

SWAP = [(0, 1), (1, 0)]

eps = 1e-06

VMEM = 62 * 2**20


def contract(left, right, over_left, over_right):
    return lax.dot_general(
        left, right, (((over_left,), (over_right,)), ((), ())), preferred_element_type=jnp.float32
    )


def slot_matrices(ids, weights, experts, capacity):
    tok_rows = ids.shape[1]
    expert = lax.broadcasted_iota(jnp.int32, (experts, tok_rows), 0)
    first, second = ids[0:1] == expert, ids[1:2] == expert
    hit = first | second
    weight = jnp.where(first, weights[0:1], jnp.where(second, weights[1:2], 0.0))
    square = (tok_rows, tok_rows)
    before = lax.broadcasted_iota(jnp.int32, square, 0) < lax.broadcasted_iota(jnp.int32, square, 1)
    rank = contract(
        jnp.where(hit, 1.0, 0.0).astype(jnp.bfloat16),
        jnp.where(before, 1.0, 0.0).astype(jnp.bfloat16),
        1,
        0,
    ).astype(jnp.int32)
    rank = jnp.where(hit, rank, capacity)
    slot = lax.broadcasted_iota(jnp.int32, (capacity, tok_rows), 0)
    select, scale, choice = [], [], []
    first, second = (jnp.where(f, 1.0, 0.0) for f in (first, second))
    for e in range(experts):
        held = rank[e : e + 1] == slot
        select.append(jnp.where(held, 1.0, 0.0))
        scale.append(jnp.where(held, weight[e : e + 1], 0.0))
        both = [jnp.where(held, f[e : e + 1], 0.0) for f in (first, second)]
        choice.append(jnp.concatenate(both, axis=1))
    return [jnp.concatenate(m, axis=0).astype(jnp.bfloat16) for m in (select, scale, choice)]


def shifted(expert, step, sign):
    return (expert // 2 + sign * (step // 2) + 4) % 4 * 2 + (expert + step) % 2


def pack_kernel(place_ref, ids_ref, w_ref, gain_ref, resid_ref, grad_ref, *out_refs):
    *normed_refs, scaled_ref, sel_ref, choice_ref, inv_ref, scale_ref, turned_ref = out_refs
    experts, capacity, block = scaled_ref.shape

    @pl.when(pl.program_id(0) == 0)
    def _():
        full = resid_ref[...].astype(jnp.float32)
        mean = jnp.mean(full * full, axis=-1, keepdims=True)
        inv_ref[...] = lax.rsqrt(mean + eps)
        select, scale, choice = slot_matrices(
            ids_ref[...], w_ref[...].astype(jnp.float32), experts, capacity
        )
        sel_ref[...] = select
        choice_ref[...] = choice
        scale_ref[...] = scale
        for step in range(experts):
            start = pl.multiple_of(shifted(place_ref[3], step, 1) * capacity, 16)
            turned_ref[step * capacity : (step + 1) * capacity] = sel_ref[pl.ds(start, capacity)]

    at = pl.ds(pl.multiple_of(pl.program_id(0) * block, block), block)
    unit = resid_ref[:, at].astype(jnp.float32) * inv_ref[...]
    normed = (unit * gain_ref[:, at]).astype(jnp.bfloat16)
    sent = contract(turned_ref[...], normed, 1, 0).astype(jnp.bfloat16)
    for step in range(experts):
        normed_refs[step][...] = sent[step * capacity : (step + 1) * capacity]
    sent = contract(scale_ref[...], grad_ref[:, at], 1, 0).astype(jnp.bfloat16)
    scaled_ref[...] = sent.reshape(experts, capacity, block)


def pack(place, ids_t, w_t, gain, resid, grad, experts, capacity, block=1024):
    rows, width = resid.shape
    args = (ids_t, w_t, gain, resid, grad)
    slots = experts * capacity
    return pl.pallas_call(
        pack_kernel,
        grid_spec=pltpu.PrefetchScalarGridSpec(
            num_scalar_prefetch=1,
            grid=(width // block,),
            in_specs=[pl.BlockSpec(a.shape, lambda j, _: (0, 0)) for a in args],
            out_specs=[pl.BlockSpec((capacity, block), lambda j, _: (0, j))] * experts
            + [
                pl.BlockSpec((experts, capacity, block), lambda j, _: (0, 0, j)),
                pl.BlockSpec((slots, rows), lambda j, _: (0, 0)),
                pl.BlockSpec((slots, 2 * rows), lambda j, _: (0, 0)),
            ],
            scratch_shapes=[
                pltpu.VMEM((rows, 1), jnp.float32),
                pltpu.VMEM((slots, rows), jnp.bfloat16),
                pltpu.VMEM((slots, rows), jnp.bfloat16),
            ],
        ),
        out_shape=[jax.ShapeDtypeStruct((capacity, width), jnp.bfloat16)] * experts
        + [
            jax.ShapeDtypeStruct((experts, capacity, width), jnp.bfloat16),
            jax.ShapeDtypeStruct((slots, rows), jnp.bfloat16),
            jax.ShapeDtypeStruct((slots, 2 * rows), jnp.bfloat16),
        ],
        compiler_params=pltpu.CompilerParams(vmem_limit_bytes=VMEM),
        cost_estimate=pl.CostEstimate(
            flops=4 * slots * rows * width, bytes_accessed=4 * slots * width, transcendentals=0
        ),
        name="pack",
    )(place, *args)


def gather_kernel(place_ref, *refs):
    *block_refs, out_ref = refs
    for step, block_ref in enumerate(block_refs):
        out_ref[shifted(place_ref[3], step, -1)] = block_ref[...]


def gather(place, blocks, block=1024):
    capacity, width = blocks[0].shape
    experts = len(blocks)
    return pl.pallas_call(
        gather_kernel,
        grid_spec=pltpu.PrefetchScalarGridSpec(
            num_scalar_prefetch=1,
            grid=(width // block,),
            in_specs=[pl.BlockSpec((capacity, block), lambda j, _: (0, j))] * experts,
            out_specs=pl.BlockSpec((experts, capacity, block), lambda j, _: (0, 0, j)),
        ),
        out_shape=jax.ShapeDtypeStruct((experts, capacity, width), jnp.bfloat16),
        compiler_params=pltpu.CompilerParams(vmem_limit_bytes=VMEM),
        cost_estimate=pl.CostEstimate(
            flops=experts * capacity * width * 256,
            bytes_accessed=4 * experts * capacity * width,
            transcendentals=0,
        ),
        name="gather",
    )(place, *blocks)


def forward_kernel(got_ref, gate_w_ref, up_w_ref, hidden_ref, gate_ref, up_ref):
    parts, capacity, width = got_ref.shape
    normed = got_ref[...].reshape(parts * capacity, width)
    gate = contract(normed, gate_w_ref[...], 1, 0)
    up = contract(normed, up_w_ref[...], 1, 0)
    sigmoid = jax.nn.sigmoid(gate)
    silu = gate * sigmoid
    hidden_ref[...] = (silu * up).astype(jnp.bfloat16)
    gate_ref[...] = up * sigmoid * (1.0 + gate * (1.0 - sigmoid))
    up_ref[...] = silu


def forward(got, w_in, block=256):
    parts, capacity, width = got.shape
    slots = parts * capacity
    hidden_width = w_in.shape[1] // 2
    steps = hidden_width // block
    out = pl.BlockSpec((slots, block), lambda j: (0, j))
    return pl.pallas_call(
        forward_kernel,
        grid=(steps,),
        in_specs=[
            pl.BlockSpec(got.shape, lambda j: (0, 0, 0)),
            pl.BlockSpec((width, block), lambda j: (0, j)),
            pl.BlockSpec((width, block), lambda j: (0, steps + j)),
        ],
        out_specs=[out] * 3,
        out_shape=[
            jax.ShapeDtypeStruct((slots, hidden_width), t)
            for t in (jnp.bfloat16, jnp.float32, jnp.float32)
        ],
        compiler_params=pltpu.CompilerParams(vmem_limit_bytes=VMEM),
        cost_estimate=pl.CostEstimate(
            flops=4 * slots * hidden_width * width,
            bytes_accessed=4 * hidden_width * width + 2 * slots * width,
            transcendentals=slots * hidden_width,
        ),
        name="forward",
    )(got, w_in, w_in)


def back_kernel(got_ref, w_ref, hidden_ref, gate_ref, up_ref, out_ref, route_ref, acc_ref):
    parts, capacity, width = got_ref.shape
    grad_hidden = contract(got_ref[...].reshape(parts * capacity, width), w_ref[...], 1, 1)
    out_ref[0] = (grad_hidden * gate_ref[...]).astype(jnp.bfloat16)
    out_ref[1] = (grad_hidden * up_ref[...]).astype(jnp.bfloat16)
    part = jnp.sum(grad_hidden * hidden_ref[...].astype(jnp.float32), axis=1, keepdims=True)

    @pl.when(pl.program_id(0) == 0)
    def _():
        acc_ref[...] = part

    @pl.when(pl.program_id(0) > 0)
    def _():
        acc_ref[...] += part

    @pl.when(pl.program_id(0) == pl.num_programs(0) - 1)
    def _():
        route_ref[...] = jnp.broadcast_to(acc_ref[...], route_ref.shape).astype(jnp.bfloat16)


def back(got, w_down, hidden, gate, up, block=256):
    parts, capacity, width = got.shape
    slots = parts * capacity
    hidden_width = w_down.shape[0]
    column = pl.BlockSpec((slots, block), lambda j: (0, j))
    return pl.pallas_call(
        back_kernel,
        grid=(hidden_width // block,),
        in_specs=[
            pl.BlockSpec(got.shape, lambda j: (0, 0, 0)),
            pl.BlockSpec((block, width), lambda j: (j, 0)),
            column,
            column,
            column,
        ],
        out_specs=[
            pl.BlockSpec((2, slots, block), lambda j: (0, 0, j)),
            pl.BlockSpec((slots, 128), lambda j: (0, 0)),
        ],
        out_shape=[
            jax.ShapeDtypeStruct((2, slots, hidden_width), jnp.bfloat16),
            jax.ShapeDtypeStruct((slots, 128), jnp.bfloat16),
        ],
        scratch_shapes=[pltpu.VMEM((slots, 1), jnp.float32)],
        compiler_params=pltpu.CompilerParams(vmem_limit_bytes=VMEM),
        cost_estimate=pl.CostEstimate(
            flops=2 * slots * hidden_width * width,
            bytes_accessed=2 * hidden_width * width + 2 * slots * width + 10 * slots * hidden_width,
            transcendentals=0,
        ),
        name="back",
    )(got, w_down, hidden, gate, up)


def turn_kernel(_, keep_ref, give_ref, keep_out, give_out):
    parts, capacity, block = keep_ref.shape
    keep_out[0] = keep_ref[...].reshape(parts * capacity, block).T.reshape(keep_out.shape[1:])
    give_out[0] = give_ref[...].reshape(parts * capacity, block).T.reshape(give_out.shape[1:])


def turn(place, got, rings, span):
    parts, capacity, width = got.shape
    slots = parts * capacity
    block = width // (4 * rings)
    steps = rings // span

    def column(half, ring, place_ref, core):
        side = jnp.where(half == 0, 1 - place_ref[0], place_ref[0])
        return (0, 0, (side * 2 + core) * steps + ring)

    out = pl.BlockSpec((1, span, block, slots), lambda half, ring, _: (half, ring, 0, 0))
    return pl.pallas_call(
        turn_kernel,
        grid_spec=pltpu.PrefetchScalarGridSpec(
            num_scalar_prefetch=1,
            grid=(2, steps),
            in_specs=[
                pl.BlockSpec(
                    (parts, capacity, span * block),
                    lambda half, ring, at: column(half, ring, at, at[1]),
                ),
                pl.BlockSpec(
                    (parts, capacity, span * block),
                    lambda half, ring, at: column(half, ring, at, 1 - at[1]),
                ),
            ],
            out_specs=[out, out],
        ),
        out_shape=[jax.ShapeDtypeStruct((2, rings, block, slots), jnp.bfloat16)] * 2,
        compiler_params=pltpu.CompilerParams(vmem_limit_bytes=VMEM),
        cost_estimate=pl.CostEstimate(
            flops=slots * width * 1024, bytes_accessed=4 * slots * width, transcendentals=0
        ),
        name="turn",
    )(place, got, got)


def both_rows(keep_ref, came_ref):
    block, slots = keep_ref.shape[2:]
    both = [r[...].reshape(2 * block, slots) for r in (keep_ref, came_ref)]
    return jnp.concatenate(both, axis=1)


def fill_right(mine_ref, theirs_ref, right_ref):
    units, slots, width = mine_ref.shape

    @pl.when(pl.program_id(0) == 0)
    def _():
        for u in range(units):
            right_ref[:slots, u * width : (u + 1) * width] = mine_ref[u]
            right_ref[slots:, u * width : (u + 1) * width] = theirs_ref[u]


def rows_kernel(_, keep_ref, came_ref, mine_ref, theirs_ref, far_ref, near_ref, right_ref):
    fill_right(mine_ref, theirs_ref, right_ref)
    rows = contract(both_rows(keep_ref, came_ref), right_ref[...], 1, 0).astype(jnp.bfloat16)
    far_ref[0] = rows[: far_ref.shape[1]]
    near_ref[0] = rows[far_ref.shape[1] :]


def weight_rows(place, keep, came, mine, theirs):
    _, rings, block, slots = keep.shape
    units, _, width = mine.shape
    left = pl.BlockSpec((2, 1, block, slots), lambda i, at: (0, lax.rem(at[2] + i, rings), 0, 0))
    right = pl.BlockSpec(mine.shape, lambda i, at: (0, 0, 0))
    out = pl.BlockSpec((1, block, units * width), lambda i, at: (i, 0, 0))
    return pl.pallas_call(
        rows_kernel,
        grid_spec=pltpu.PrefetchScalarGridSpec(
            num_scalar_prefetch=1,
            grid=(rings,),
            in_specs=[left, left, right, right],
            out_specs=[out, out],
            scratch_shapes=[pltpu.VMEM((2 * slots, units * width), jnp.bfloat16)],
        ),
        out_shape=[jax.ShapeDtypeStruct((rings, block, units * width), jnp.bfloat16)] * 2,
        compiler_params=pltpu.CompilerParams(vmem_limit_bytes=VMEM),
        cost_estimate=pl.CostEstimate(
            flops=8 * rings * block * mine.size,
            bytes_accessed=4 * mine.size + 4 * rings * block * (2 * slots + units * width),
            transcendentals=0,
        ),
    )(place, keep, came, mine, theirs)


SEND_ORDER = (2, 1, 3, 0)


def ring_at(step):
    ring = SEND_ORDER[-1]
    for at, value in enumerate(SEND_ORDER[:-1]):
        ring = jnp.where(step == at, value, ring)
    return ring


def messages_kernel(_, keep_ref, came_ref, mine_ref, theirs_ref, *out_refs):
    *out_refs, right_ref = out_refs
    block = keep_ref.shape[2]
    fill_right(mine_ref, theirs_ref, right_ref)
    for at in range(len(SEND_ORDER)):

        @pl.when(pl.program_id(0) == at)
        def _():
            rows = contract(both_rows(keep_ref, came_ref), right_ref[...], 1, 0)
            rows = rows.astype(jnp.bfloat16)
            out_refs[2 * at][0] = rows[:block]
            out_refs[2 * at + 1][0] = rows[block:]


def weight_messages(place, keep, came, mine, theirs):
    _, rings, block, slots = keep.shape
    units, _, width = mine.shape
    left = pl.BlockSpec(
        (2, 1, block, slots), lambda i, at: (0, lax.rem(at[2] + ring_at(i), rings), 0, 0)
    )
    right = pl.BlockSpec(mine.shape, lambda i, at: (0, 0, 0))
    outs = pl.pallas_call(
        messages_kernel,
        grid_spec=pltpu.PrefetchScalarGridSpec(
            num_scalar_prefetch=1,
            grid=(rings,),
            in_specs=[left, left, right, right],
            out_specs=[pl.BlockSpec((1, block, units * width), lambda i, at: (0, 0, 0))]
            * (2 * rings),
            scratch_shapes=[pltpu.VMEM((2 * slots, units * width), jnp.bfloat16)],
        ),
        out_shape=[jax.ShapeDtypeStruct((1, block, units * width), jnp.bfloat16)] * (2 * rings),
        compiler_params=pltpu.CompilerParams(vmem_limit_bytes=VMEM),
        cost_estimate=pl.CostEstimate(
            flops=8 * rings * block * mine.size,
            bytes_accessed=4 * mine.size + 4 * rings * block * (2 * slots + units * width),
            transcendentals=0,
        ),
        name="grad_in",
    )(place, keep, came, mine, theirs)
    far = {ring: outs[2 * k] for k, ring in enumerate(SEND_ORDER)}
    near = {ring: outs[2 * k + 1] for k, ring in enumerate(SEND_ORDER)}
    return far, near


def slot_kernel(grads_ref, w_ref, route_ref, out_ref):
    width = grads_ref.shape[2]
    block = w_ref.shape[0]
    rows = contract(grads_ref[0], w_ref[:, :width], 1, 1) + contract(
        grads_ref[1], w_ref[:, width:], 1, 1
    )
    at = pl.ds(pl.multiple_of(pl.program_id(0) * block, block), block)
    out_ref[:, :, at] = rows.astype(jnp.bfloat16).reshape(out_ref.shape[:2] + (block,))

    @pl.when(pl.program_id(0) == 0)
    def _():
        lanes = route_ref.shape[1]
        out_ref[:, :, out_ref.shape[2] - lanes :] = route_ref[...].reshape(
            out_ref.shape[:2] + (lanes,)
        )


def slot_rows(grads, w_in, route, parts, block=1024):
    _, slots, hidden_width = grads.shape
    width = w_in.shape[0]
    shape = (parts, slots // parts, width + route.shape[1])
    return pl.pallas_call(
        slot_kernel,
        grid=(width // block,),
        in_specs=[
            pl.BlockSpec(grads.shape, lambda j: (0, 0, 0)),
            pl.BlockSpec((block, 2 * hidden_width), lambda j: (j, 0)),
            pl.BlockSpec(route.shape, lambda j: (0, 0)),
        ],
        out_specs=pl.BlockSpec(shape, lambda j: (0, 0, 0)),
        out_shape=jax.ShapeDtypeStruct(shape, jnp.bfloat16),
        compiler_params=pltpu.CompilerParams(vmem_limit_bytes=VMEM),
        cost_estimate=pl.CostEstimate(
            flops=4 * slots * hidden_width * width,
            bytes_accessed=4 * hidden_width * width + 2 * slots * width,
            transcendentals=0,
        ),
        name="slot_rows",
    )(grads, w_in, route)


def displaced(rows, step):
    experts = lax.axis_size("expert")
    pairs = [
        (side * experts + e, (side + step) % 2 * experts + shifted(e, step, 1))
        for side in range(2)
        for e in range(experts)
    ]
    return lax.ppermute(rows, ("dp_0", "expert"), pairs)


def added(*terms):
    return sum(t.astype(jnp.float32) for t in terms)


def ring_sum(low, high):
    size = lax.axis_size("ulysses")
    ahead = [(i, (i + 1) % size) for i in range(size)]
    behind = [(i, (i - 1) % size) for i in range(size)]
    low_two = lax.ppermute(low[2], "ulysses", ahead)
    high_two = lax.ppermute(high[2], "ulysses", behind)
    high_side = lax.ppermute(high[1], "ulysses", ahead)
    low_side = lax.ppermute(low[3], "ulysses", behind)
    low_both = added(low[1], low_two).astype(jnp.bfloat16)
    high_both = added(high[3], high_two).astype(jnp.bfloat16)
    low_last = lax.ppermute(low_both, "ulysses", ahead)
    high_last = lax.ppermute(high_both, "ulysses", behind)
    sums = added(low[0], low_last, low_side), added(high[0], high_last, high_side)
    return sums, low_both, high_both


def exchange(rows):
    experts = lax.axis_size("expert")
    groups = [[(g ^ (e & 1)) * experts + e for e in range(experts)] for g in range(2)]
    return lax.all_to_all(
        rows,
        ("dp_0", "expert"),
        split_axis=0,
        concat_axis=0,
        axis_index_groups=groups,
        tiled=True,
    )


def per_device(residual, norm_gain, grad_out, expert_ids, route_weights, weight_in, weight_down):
    tok_rows, width = residual.shape
    topk = expert_ids.shape[1]
    experts = lax.axis_size("expert")
    capacity = min(tok_rows, 3 * tok_rows * topk // (2 * experts))
    slot_total = experts * capacity
    rings = lax.axis_size("ulysses")
    block = width // (4 * rings)
    span = 2 if rings % 2 == 0 else 1
    side = lax.axis_index("dp_0")
    core = lax.axis_index("dp_1")
    ids_t = expert_ids.T
    weights_t = route_weights.T
    place, residual = lax.optimization_barrier(
        (
            jnp.stack([side, core, lax.axis_index("ulysses"), lax.axis_index("expert")]).astype(
                jnp.int32
            ),
            residual,
        )
    )

    *send_normed, send_scaled, select, choice = pack(
        place, ids_t, weights_t, norm_gain[None], residual, grad_out, experts, capacity
    )
    blocks = send_normed[:1] + [displaced(send_normed[k], k) for k in range(1, experts)]
    got_scaled = exchange(send_scaled)
    got_normed = gather(place, blocks)
    w_in = weight_in[0]
    w_down = weight_down[0]
    keep_normed, give_normed = turn(place, got_normed, rings, span)
    came_normed = lax.ppermute(give_normed, "dp_1", SWAP)
    hidden, gate, up = forward(got_normed, w_in)
    their_hidden = lax.ppermute(hidden, "dp_1", SWAP)
    mine, route = back(got_scaled, w_down, hidden, gate, up)
    theirs = lax.ppermute(mine, "dp_1", SWAP)
    got_scaled, mine, route = lax.optimization_barrier((got_scaled, mine, route))
    keep_scaled, give_scaled = turn(place, got_scaled, rings, span)
    came_scaled = lax.ppermute(give_scaled, "dp_1", SWAP)
    keep_normed, keep_scaled = lax.optimization_barrier((keep_normed, keep_scaled))
    far, near = weight_messages(place, keep_normed, came_normed, mine, theirs)
    keep_scaled, _ = lax.optimization_barrier((keep_scaled, near[0]))
    far_down, near_down = weight_rows(
        place, keep_scaled, came_scaled, hidden[None], their_hidden[None]
    )
    came_down = lax.ppermute(far_down, "dp_0", SWAP)
    (far_in, near_in), far_both, near_both = ring_sum(far, near)
    came_in = lax.ppermute(far_in.astype(jnp.bfloat16), "dp_0", SWAP)
    came_down, _, _ = lax.optimization_barrier((came_down, far_both, near_both))
    part_down = added(near_down, came_down).astype(jnp.bfloat16)
    upper = {r: part_down[r, : block // 2] for r in range(rings)}
    lower = {r: part_down[r, block // 2 :] for r in range(rings)}
    halves_down, _, _ = ring_sum(upper, lower)
    grad_down = jnp.concatenate(halves_down, axis=0)[None]

    mine, route, _ = lax.optimization_barrier((mine, route, near_down))
    slot_normed = slot_rows(mine, w_in, route, experts)
    returned = exchange(slot_normed).reshape(slot_total, -1)
    resid = residual.astype(jnp.float32)
    inv_rms = lax.rsqrt(jnp.mean(resid * resid, axis=-1, keepdims=True) + eps)
    unit_rows = resid * inv_rms
    grad_normed = contract(select, returned[:, :width], 0, 0)
    route_t = contract(choice, returned[:, width:], 0, 0)[:, 0].reshape(topk, tok_rows)
    route_grad = (route_t / weights_t.astype(jnp.float32)).astype(jnp.bfloat16).T
    scaled_normed = grad_normed * norm_gain
    branch = inv_rms * (
        scaled_normed - unit_rows * jnp.mean(scaled_normed * unit_rows, axis=-1, keepdims=True)
    )
    grad_residual = (grad_out.astype(jnp.float32) + branch).astype(jnp.bfloat16)
    came_in, _ = lax.optimization_barrier((came_in, grad_residual))
    grad_in = near_in + came_in.astype(jnp.float32)
    return (grad_residual, route_grad, grad_in, grad_down)


def solution(mesh):
    finer = Mesh(
        mesh.devices.reshape(2, 2, mesh.shape["ulysses"], mesh.shape["expert"]),
        ("dp_0", "dp_1", "ulysses", "expert"),
    )
    return jax.shard_map(
        per_device,
        mesh=finer,
        in_specs=(
            P(DP_ULYSSES_EXPERT, None),
            P(),
            P(DP_ULYSSES_EXPERT, None),
            P(DP_ULYSSES_EXPERT, None),
            P(DP_ULYSSES_EXPERT, None),
            P("expert", None, None),
            P("expert", None, None),
        ),
        out_specs=(
            P(DP_ULYSSES_EXPERT, None),
            P(DP_ULYSSES_EXPERT, None),
            P("expert", DP_ULYSSES, None),
            P("expert", DP_ULYSSES, None),
        ),
        check_vma=False,
    )
```

```python
import jax
import jax.numpy as jnp
from jax import lax
from jax.experimental import pallas as pl
from jax.experimental.pallas import tpu as pltpu
from jax.sharding import Mesh
from jax.sharding import PartitionSpec as P


DP_ULYSSES = ("dp_0", "dp_1", "ulysses")
DP_ULYSSES_EXPERT = ("dp_0", "dp_1", "ulysses", "expert")

SWAP = [(0, 1), (1, 0)]

eps = 1e-06

VMEM = 66_000_000


def contract(left, right, over_left, over_right):
    return lax.dot_general(
        left, right, (((over_left,), (over_right,)), ((), ())), preferred_element_type=jnp.float32
    )


def slot_matrices(ids, weights, experts, capacity):
    tok_rows = ids.shape[1]
    expert = lax.broadcasted_iota(jnp.int32, (experts, tok_rows), 0)
    first, second = ids[0:1] == expert, ids[1:2] == expert
    hit = first | second
    weight = jnp.where(first, weights[0:1], jnp.where(second, weights[1:2], 0.0))
    square = (tok_rows, tok_rows)
    before = lax.broadcasted_iota(jnp.int32, square, 0) < lax.broadcasted_iota(jnp.int32, square, 1)
    rank = contract(
        jnp.where(hit, 1.0, 0.0).astype(jnp.bfloat16),
        jnp.where(before, 1.0, 0.0).astype(jnp.bfloat16),
        1,
        0,
    ).astype(jnp.int32)
    rank = jnp.where(hit, rank, capacity)
    slot = lax.broadcasted_iota(jnp.int32, (capacity, tok_rows), 0)
    select, scale, choice = [], [], []
    first, second = (jnp.where(f, 1.0, 0.0) for f in (first, second))
    for e in range(experts):
        held = rank[e : e + 1] == slot
        select.append(jnp.where(held, 1.0, 0.0))
        scale.append(jnp.where(held, weight[e : e + 1], 0.0))
        both = [jnp.where(held, f[e : e + 1], 0.0) for f in (first, second)]
        choice.append(jnp.concatenate(both, axis=1))
    return [jnp.concatenate(m, axis=0).astype(jnp.bfloat16) for m in (select, scale, choice)]


def shifted(expert, step, sign):
    return (expert // 2 + sign * (step // 2) + 4) % 4 * 2 + (expert + step) % 2


def pack_kernel(place_ref, ids_ref, w_ref, gain_ref, resid_ref, grad_ref, *out_refs):
    *normed_refs, scaled_ref, sel_ref, choice_ref, inv_ref, scale_ref, turned_ref = out_refs
    experts, capacity, block = scaled_ref.shape

    @pl.when(pl.program_id(0) == 0)
    def _():
        full = resid_ref[...].astype(jnp.float32)
        mean = jnp.mean(full * full, axis=-1, keepdims=True)
        inv_ref[...] = lax.rsqrt(mean + eps)
        select, scale, choice = slot_matrices(
            ids_ref[...], w_ref[...].astype(jnp.float32), experts, capacity
        )
        sel_ref[...] = select
        choice_ref[...] = choice
        scale_ref[...] = scale
        for step in range(experts):
            start = pl.multiple_of(shifted(place_ref[3], step, 1) * capacity, 16)
            turned_ref[step * capacity : (step + 1) * capacity] = sel_ref[pl.ds(start, capacity)]

    at = pl.ds(pl.multiple_of(pl.program_id(0) * block, block), block)
    unit = resid_ref[:, at].astype(jnp.float32) * inv_ref[...]
    normed = (unit * gain_ref[:, at]).astype(jnp.bfloat16)
    sent = contract(turned_ref[...], normed, 1, 0).astype(jnp.bfloat16)
    for step in range(experts):
        normed_refs[step][...] = sent[step * capacity : (step + 1) * capacity]
    sent = contract(scale_ref[...], grad_ref[:, at], 1, 0).astype(jnp.bfloat16)
    scaled_ref[...] = sent.reshape(experts, capacity, block)


def pack(place, ids_t, w_t, gain, resid, grad, experts, capacity, block=1024):
    rows, width = resid.shape
    args = (ids_t, w_t, gain, resid, grad)
    slots = experts * capacity
    return pl.pallas_call(
        pack_kernel,
        grid_spec=pltpu.PrefetchScalarGridSpec(
            num_scalar_prefetch=1,
            grid=(width // block,),
            in_specs=[pl.BlockSpec(a.shape, lambda j, _: (0, 0)) for a in args],
            out_specs=[pl.BlockSpec((capacity, block), lambda j, _: (0, j))] * experts
            + [
                pl.BlockSpec((experts, capacity, block), lambda j, _: (0, 0, j)),
                pl.BlockSpec((slots, rows), lambda j, _: (0, 0)),
                pl.BlockSpec((slots, 2 * rows), lambda j, _: (0, 0)),
            ],
            scratch_shapes=[
                pltpu.VMEM((rows, 1), jnp.float32),
                pltpu.VMEM((slots, rows), jnp.bfloat16),
                pltpu.VMEM((slots, rows), jnp.bfloat16),
            ],
        ),
        out_shape=[jax.ShapeDtypeStruct((capacity, width), jnp.bfloat16)] * experts
        + [
            jax.ShapeDtypeStruct((experts, capacity, width), jnp.bfloat16),
            jax.ShapeDtypeStruct((slots, rows), jnp.bfloat16),
            jax.ShapeDtypeStruct((slots, 2 * rows), jnp.bfloat16),
        ],
        compiler_params=pltpu.CompilerParams(vmem_limit_bytes=VMEM),
        cost_estimate=pl.CostEstimate(
            flops=4 * slots * rows * width, bytes_accessed=4 * slots * width, transcendentals=0
        ),
        name="pack",
    )(place, *args)


def gather_kernel(place_ref, *refs):
    *block_refs, out_ref = refs
    for step, block_ref in enumerate(block_refs):
        out_ref[shifted(place_ref[3], step, -1)] = block_ref[...]


def gather(place, blocks, block=1024):
    capacity, width = blocks[0].shape
    experts = len(blocks)
    return pl.pallas_call(
        gather_kernel,
        grid_spec=pltpu.PrefetchScalarGridSpec(
            num_scalar_prefetch=1,
            grid=(width // block,),
            in_specs=[pl.BlockSpec((capacity, block), lambda j, _: (0, j))] * experts,
            out_specs=pl.BlockSpec((experts, capacity, block), lambda j, _: (0, 0, j)),
        ),
        out_shape=jax.ShapeDtypeStruct((experts, capacity, width), jnp.bfloat16),
        compiler_params=pltpu.CompilerParams(vmem_limit_bytes=VMEM),
        cost_estimate=pl.CostEstimate(
            flops=experts * capacity * width * 256,
            bytes_accessed=4 * experts * capacity * width,
            transcendentals=0,
        ),
        name="gather",
    )(place, *blocks)


def forward_kernel(got_ref, gate_w_ref, up_w_ref, hidden_ref, gate_ref, up_ref):
    parts, capacity, width = got_ref.shape
    normed = got_ref[...].reshape(parts * capacity, width)
    gate = contract(normed, gate_w_ref[...], 1, 0)
    up = contract(normed, up_w_ref[...], 1, 0)
    sigmoid = jax.nn.sigmoid(gate)
    silu = gate * sigmoid
    hidden_ref[...] = (silu * up).astype(jnp.bfloat16)
    gate_ref[...] = up * sigmoid * (1.0 + gate * (1.0 - sigmoid))
    up_ref[...] = silu


def forward(got, w_in, block=256):
    parts, capacity, width = got.shape
    slots = parts * capacity
    hidden_width = w_in.shape[1] // 2
    steps = hidden_width // block
    out = pl.BlockSpec((slots, block), lambda j: (0, j))
    return pl.pallas_call(
        forward_kernel,
        grid=(steps,),
        in_specs=[
            pl.BlockSpec(got.shape, lambda j: (0, 0, 0)),
            pl.BlockSpec((width, block), lambda j: (0, j)),
            pl.BlockSpec((width, block), lambda j: (0, steps + j)),
        ],
        out_specs=[out] * 3,
        out_shape=[
            jax.ShapeDtypeStruct((slots, hidden_width), t)
            for t in (jnp.bfloat16, jnp.float32, jnp.float32)
        ],
        compiler_params=pltpu.CompilerParams(vmem_limit_bytes=VMEM),
        cost_estimate=pl.CostEstimate(
            flops=4 * slots * hidden_width * width,
            bytes_accessed=4 * hidden_width * width + 2 * slots * width,
            transcendentals=slots * hidden_width,
        ),
        name="forward",
    )(got, w_in, w_in)


def back_kernel(got_ref, w_ref, hidden_ref, gate_ref, up_ref, out_ref, route_ref, acc_ref):
    parts, capacity, width = got_ref.shape
    grad_hidden = contract(got_ref[...].reshape(parts * capacity, width), w_ref[...], 1, 1)
    out_ref[0] = (grad_hidden * gate_ref[...]).astype(jnp.bfloat16)
    out_ref[1] = (grad_hidden * up_ref[...]).astype(jnp.bfloat16)
    part = jnp.sum(grad_hidden * hidden_ref[...].astype(jnp.float32), axis=1, keepdims=True)

    @pl.when(pl.program_id(0) == 0)
    def _():
        acc_ref[...] = part

    @pl.when(pl.program_id(0) > 0)
    def _():
        acc_ref[...] += part

    @pl.when(pl.program_id(0) == pl.num_programs(0) - 1)
    def _():
        route_ref[...] = jnp.broadcast_to(acc_ref[...], route_ref.shape).astype(jnp.bfloat16)


def back(got, w_down, hidden, gate, up, block=384):
    parts, capacity, width = got.shape
    slots = parts * capacity
    hidden_width = w_down.shape[0]
    column = pl.BlockSpec((slots, block), lambda j: (0, j))
    return pl.pallas_call(
        back_kernel,
        grid=(hidden_width // block,),
        in_specs=[
            pl.BlockSpec(got.shape, lambda j: (0, 0, 0)),
            pl.BlockSpec((block, width), lambda j: (j, 0)),
            column,
            column,
            column,
        ],
        out_specs=[
            pl.BlockSpec((2, slots, block), lambda j: (0, 0, j)),
            pl.BlockSpec((slots, 128), lambda j: (0, 0)),
        ],
        out_shape=[
            jax.ShapeDtypeStruct((2, slots, hidden_width), jnp.bfloat16),
            jax.ShapeDtypeStruct((slots, 128), jnp.bfloat16),
        ],
        scratch_shapes=[pltpu.VMEM((slots, 1), jnp.float32)],
        compiler_params=pltpu.CompilerParams(vmem_limit_bytes=VMEM),
        cost_estimate=pl.CostEstimate(
            flops=2 * slots * hidden_width * width,
            bytes_accessed=2 * hidden_width * width + 2 * slots * width + 10 * slots * hidden_width,
            transcendentals=0,
        ),
        name="back",
    )(got, w_down, hidden, gate, up)


def turn_kernel(_, keep_ref, give_ref, keep_out, give_out):
    parts, capacity, block = keep_ref.shape
    keep_out[0] = keep_ref[...].reshape(parts * capacity, block).T.reshape(keep_out.shape[1:])
    give_out[0] = give_ref[...].reshape(parts * capacity, block).T.reshape(give_out.shape[1:])


def turn(place, got, rings, span):
    parts, capacity, width = got.shape
    slots = parts * capacity
    block = width // (4 * rings)
    steps = rings // span

    def column(half, ring, place_ref, core):
        side = jnp.where(half == 0, 1 - place_ref[0], place_ref[0])
        return (0, 0, (side * 2 + core) * steps + ring)

    out = pl.BlockSpec((1, span, block, slots), lambda half, ring, _: (half, ring, 0, 0))
    return pl.pallas_call(
        turn_kernel,
        grid_spec=pltpu.PrefetchScalarGridSpec(
            num_scalar_prefetch=1,
            grid=(2, steps),
            in_specs=[
                pl.BlockSpec(
                    (parts, capacity, span * block),
                    lambda half, ring, at: column(half, ring, at, at[1]),
                ),
                pl.BlockSpec(
                    (parts, capacity, span * block),
                    lambda half, ring, at: column(half, ring, at, 1 - at[1]),
                ),
            ],
            out_specs=[out, out],
        ),
        out_shape=[jax.ShapeDtypeStruct((2, rings, block, slots), jnp.bfloat16)] * 2,
        compiler_params=pltpu.CompilerParams(vmem_limit_bytes=VMEM),
        cost_estimate=pl.CostEstimate(
            flops=slots * width * 1024, bytes_accessed=4 * slots * width, transcendentals=0
        ),
        name="turn",
    )(place, got, got)


def both_rows(keep_ref, came_ref):
    block, slots = keep_ref.shape[2:]
    both = [r[...].reshape(2 * block, slots) for r in (keep_ref, came_ref)]
    return jnp.concatenate(both, axis=1)


def fill_right(mine_ref, theirs_ref, right_ref):
    units, slots, width = mine_ref.shape

    @pl.when(pl.program_id(0) == 0)
    def _():
        for u in range(units):
            right_ref[:slots, u * width : (u + 1) * width] = mine_ref[u]
            right_ref[slots:, u * width : (u + 1) * width] = theirs_ref[u]


def rows_kernel(_, keep_ref, came_ref, mine_ref, theirs_ref, far_ref, near_ref, right_ref):
    fill_right(mine_ref, theirs_ref, right_ref)
    rows = contract(both_rows(keep_ref, came_ref), right_ref[...], 1, 0).astype(jnp.bfloat16)
    far_ref[0] = rows[: far_ref.shape[1]]
    near_ref[0] = rows[far_ref.shape[1] :]


def weight_rows(place, keep, came, mine, theirs):
    _, rings, block, slots = keep.shape
    units, _, width = mine.shape
    left = pl.BlockSpec((2, 1, block, slots), lambda i, at: (0, lax.rem(at[2] + i, rings), 0, 0))
    right = pl.BlockSpec(mine.shape, lambda i, at: (0, 0, 0))
    out = pl.BlockSpec((1, block, units * width), lambda i, at: (i, 0, 0))
    return pl.pallas_call(
        rows_kernel,
        grid_spec=pltpu.PrefetchScalarGridSpec(
            num_scalar_prefetch=1,
            grid=(rings,),
            in_specs=[left, left, right, right],
            out_specs=[out, out],
            scratch_shapes=[pltpu.VMEM((2 * slots, units * width), jnp.bfloat16)],
        ),
        out_shape=[jax.ShapeDtypeStruct((rings, block, units * width), jnp.bfloat16)] * 2,
        compiler_params=pltpu.CompilerParams(vmem_limit_bytes=VMEM),
        cost_estimate=pl.CostEstimate(
            flops=8 * rings * block * mine.size,
            bytes_accessed=4 * mine.size + 4 * rings * block * (2 * slots + units * width),
            transcendentals=0,
        ),
    )(place, keep, came, mine, theirs)


SEND_ORDER = (2, 1, 3, 0)


def ring_at(step):
    ring = SEND_ORDER[-1]
    for at, value in enumerate(SEND_ORDER[:-1]):
        ring = jnp.where(step == at, value, ring)
    return ring


def messages_kernel(_, keep_ref, came_ref, mine_ref, theirs_ref, *out_refs):
    *out_refs, right_ref = out_refs
    block = keep_ref.shape[2]
    fill_right(mine_ref, theirs_ref, right_ref)
    for at in range(len(SEND_ORDER)):

        @pl.when(pl.program_id(0) == at)
        def _():
            rows = contract(both_rows(keep_ref, came_ref), right_ref[...], 1, 0)
            rows = rows.astype(jnp.bfloat16)
            out_refs[2 * at][0] = rows[:block]
            out_refs[2 * at + 1][0] = rows[block:]


def weight_messages(place, keep, came, mine, theirs):
    _, rings, block, slots = keep.shape
    units, _, width = mine.shape
    left = pl.BlockSpec(
        (2, 1, block, slots), lambda i, at: (0, lax.rem(at[2] + ring_at(i), rings), 0, 0)
    )
    right = pl.BlockSpec(mine.shape, lambda i, at: (0, 0, 0))
    outs = pl.pallas_call(
        messages_kernel,
        grid_spec=pltpu.PrefetchScalarGridSpec(
            num_scalar_prefetch=1,
            grid=(rings,),
            in_specs=[left, left, right, right],
            out_specs=[pl.BlockSpec((1, block, units * width), lambda i, at: (0, 0, 0))]
            * (2 * rings),
            scratch_shapes=[pltpu.VMEM((2 * slots, units * width), jnp.bfloat16)],
        ),
        out_shape=[jax.ShapeDtypeStruct((1, block, units * width), jnp.bfloat16)] * (2 * rings),
        compiler_params=pltpu.CompilerParams(vmem_limit_bytes=VMEM),
        cost_estimate=pl.CostEstimate(
            flops=8 * rings * block * mine.size,
            bytes_accessed=4 * mine.size + 4 * rings * block * (2 * slots + units * width),
            transcendentals=0,
        ),
        name="grad_in",
    )(place, keep, came, mine, theirs)
    far = {ring: outs[2 * k] for k, ring in enumerate(SEND_ORDER)}
    near = {ring: outs[2 * k + 1] for k, ring in enumerate(SEND_ORDER)}
    return far, near


def slot_kernel(grads_ref, w_ref, route_ref, out_ref, both_ref):
    width = grads_ref.shape[2]
    block = w_ref.shape[0]

    @pl.when(pl.program_id(0) == 0)
    def _():
        both_ref[:, :width] = grads_ref[0]
        both_ref[:, width:] = grads_ref[1]

    rows = contract(both_ref[...], w_ref[...], 1, 1)
    at = pl.ds(pl.multiple_of(pl.program_id(0) * block, block), block)
    out_ref[:, :, at] = rows.astype(jnp.bfloat16).reshape(out_ref.shape[:2] + (block,))

    @pl.when(pl.program_id(0) == 0)
    def _():
        lanes = route_ref.shape[1]
        out_ref[:, :, out_ref.shape[2] - lanes :] = route_ref[...].reshape(
            out_ref.shape[:2] + (lanes,)
        )


def slot_rows(grads, w_in, route, parts, block=512):
    _, slots, hidden_width = grads.shape
    width = w_in.shape[0]
    shape = (parts, slots // parts, width + route.shape[1])
    return pl.pallas_call(
        slot_kernel,
        grid=(width // block,),
        in_specs=[
            pl.BlockSpec(grads.shape, lambda j: (0, 0, 0)),
            pl.BlockSpec((block, 2 * hidden_width), lambda j: (j, 0)),
            pl.BlockSpec(route.shape, lambda j: (0, 0)),
        ],
        out_specs=pl.BlockSpec(shape, lambda j: (0, 0, 0)),
        out_shape=jax.ShapeDtypeStruct(shape, jnp.bfloat16),
        scratch_shapes=[pltpu.VMEM((slots, 2 * hidden_width), jnp.bfloat16)],
        compiler_params=pltpu.CompilerParams(vmem_limit_bytes=VMEM),
        cost_estimate=pl.CostEstimate(
            flops=4 * slots * hidden_width * width,
            bytes_accessed=4 * hidden_width * width + 2 * slots * width,
            transcendentals=0,
        ),
        name="slot_rows",
    )(grads, w_in, route)


def displaced(rows, step):
    experts = lax.axis_size("expert")
    pairs = [
        (side * experts + e, (side + step) % 2 * experts + shifted(e, step, 1))
        for side in range(2)
        for e in range(experts)
    ]
    return lax.ppermute(rows, ("dp_0", "expert"), pairs)


def added(*terms):
    return sum(t.astype(jnp.float32) for t in terms)


def ring_sum(low, high):
    size = lax.axis_size("ulysses")
    ahead = [(i, (i + 1) % size) for i in range(size)]
    behind = [(i, (i - 1) % size) for i in range(size)]
    low_two = lax.ppermute(low[2], "ulysses", ahead)
    high_two = lax.ppermute(high[2], "ulysses", behind)
    high_side = lax.ppermute(high[1], "ulysses", ahead)
    low_side = lax.ppermute(low[3], "ulysses", behind)
    low_both = added(low[1], low_two).astype(jnp.bfloat16)
    high_both = added(high[3], high_two).astype(jnp.bfloat16)
    low_last = lax.ppermute(low_both, "ulysses", ahead)
    high_last = lax.ppermute(high_both, "ulysses", behind)
    sums = added(low[0], low_last, low_side), added(high[0], high_last, high_side)
    return sums, low_both, high_both


def exchange(rows):
    experts = lax.axis_size("expert")
    groups = [[(g ^ (e & 1)) * experts + e for e in range(experts)] for g in range(2)]
    return lax.all_to_all(
        rows,
        ("dp_0", "expert"),
        split_axis=0,
        concat_axis=0,
        axis_index_groups=groups,
        tiled=True,
    )


def per_device(residual, norm_gain, grad_out, expert_ids, route_weights, weight_in, weight_down):
    tok_rows, width = residual.shape
    topk = expert_ids.shape[1]
    experts = lax.axis_size("expert")
    capacity = min(tok_rows, 3 * tok_rows * topk // (2 * experts))
    slot_total = experts * capacity
    rings = lax.axis_size("ulysses")
    block = width // (4 * rings)
    span = 2 if rings % 2 == 0 else 1
    side = lax.axis_index("dp_0")
    core = lax.axis_index("dp_1")
    ids_t = expert_ids.T
    weights_t = route_weights.T
    place, residual = lax.optimization_barrier(
        (
            jnp.stack([side, core, lax.axis_index("ulysses"), lax.axis_index("expert")]).astype(
                jnp.int32
            ),
            residual,
        )
    )

    *send_normed, send_scaled, select, choice = pack(
        place, ids_t, weights_t, norm_gain[None], residual, grad_out, experts, capacity
    )
    blocks = send_normed[:1] + [displaced(send_normed[k], k) for k in range(1, experts)]
    got_scaled = exchange(send_scaled)
    got_normed = gather(place, blocks)
    w_in = weight_in[0]
    w_down = weight_down[0]
    keep_normed, give_normed = turn(place, got_normed, rings, span)
    came_normed = lax.ppermute(give_normed, "dp_1", SWAP)
    hidden, gate, up = forward(got_normed, w_in)
    their_hidden = lax.ppermute(hidden, "dp_1", SWAP)
    mine, route = back(got_scaled, w_down, hidden, gate, up)
    theirs = lax.ppermute(mine, "dp_1", SWAP)
    got_scaled, mine, route = lax.optimization_barrier((got_scaled, mine, route))
    keep_scaled, give_scaled = turn(place, got_scaled, rings, span)
    came_scaled = lax.ppermute(give_scaled, "dp_1", SWAP)
    keep_normed, keep_scaled = lax.optimization_barrier((keep_normed, keep_scaled))
    far, near = weight_messages(place, keep_normed, came_normed, mine, theirs)
    keep_scaled, _ = lax.optimization_barrier((keep_scaled, near[0]))
    far_down, near_down = weight_rows(
        place, keep_scaled, came_scaled, hidden[None], their_hidden[None]
    )
    came_down = lax.ppermute(far_down, "dp_0", SWAP)
    (far_in, near_in), far_both, near_both = ring_sum(far, near)
    came_in = lax.ppermute(far_in.astype(jnp.bfloat16), "dp_0", SWAP)
    came_down, _, _ = lax.optimization_barrier((came_down, far_both, near_both))
    part_down = added(near_down, came_down).astype(jnp.bfloat16)
    upper = {r: part_down[r, : block // 2] for r in range(rings)}
    lower = {r: part_down[r, block // 2 :] for r in range(rings)}
    halves_down, _, _ = ring_sum(upper, lower)
    grad_down = jnp.concatenate(halves_down, axis=0)[None]

    mine, route, _ = lax.optimization_barrier((mine, route, near_down))
    slot_normed = slot_rows(mine, w_in, route, experts)
    returned = exchange(slot_normed).reshape(slot_total, -1)
    resid = residual.astype(jnp.float32)
    inv_rms = lax.rsqrt(jnp.mean(resid * resid, axis=-1, keepdims=True) + eps)
    unit_rows = resid * inv_rms
    grad_normed = contract(select, returned[:, :width], 0, 0)
    route_t = contract(choice, returned[:, width:], 0, 0)[:, 0].reshape(topk, tok_rows)
    route_grad = (route_t / weights_t.astype(jnp.float32)).astype(jnp.bfloat16).T
    scaled_normed = grad_normed * norm_gain
    branch = inv_rms * (
        scaled_normed - unit_rows * jnp.mean(scaled_normed * unit_rows, axis=-1, keepdims=True)
    )
    grad_residual = (grad_out.astype(jnp.float32) + branch).astype(jnp.bfloat16)
    near_in = lax.optimization_barrier(near_in)
    came_in, _ = lax.optimization_barrier((came_in, grad_residual))
    grad_in = near_in + came_in.astype(jnp.float32)
    return (grad_residual, route_grad, grad_in, grad_down)


def solution(mesh):
    finer = Mesh(
        mesh.devices.reshape(2, 2, mesh.shape["ulysses"], mesh.shape["expert"]),
        ("dp_0", "dp_1", "ulysses", "expert"),
    )
    return jax.shard_map(
        per_device,
        mesh=finer,
        in_specs=(
            P(DP_ULYSSES_EXPERT, None),
            P(),
            P(DP_ULYSSES_EXPERT, None),
            P(DP_ULYSSES_EXPERT, None),
            P(DP_ULYSSES_EXPERT, None),
            P("expert", None, None),
            P("expert", None, None),
        ),
        out_specs=(
            P(DP_ULYSSES_EXPERT, None),
            P(DP_ULYSSES_EXPERT, None),
            P("expert", DP_ULYSSES, None),
            P("expert", DP_ULYSSES, None),
        ),
        check_vma=False,
    )
```
